32 devices in a mesh: bump: 4 (over y, core), nx: 2 (over x), ny: 4 (over z).
Axes of the slice: x: 2, y: 2, z: 4, core: 2. Of those that a mesh axis runs over, the one named last changes fastest.
Arguments:
- payoff: float32 [262144], P(('nx', 'ny')), may hold values from -6 to 6
- positions: float32 [262144], P(('nx', 'ny')), may hold values from -20 to 20
- tables: float32 [8, 5, 262144], P('bump', None, ('nx', 'ny')), may hold values from 0.02 to 1, as said below
- offsets: int32 [8, 1024], P(None, ('nx', 'ny')), may hold values from -1 to 1
- vol_curve: float32 [8], replicated, may hold values from 0.5 to 1.2
- bucket: int32 [64], P('bump'), may hold values from 0 to 7
- bump_size: float32 [64], P('bump'), may hold values from 0.1 to 0.4
Outputs:
- bumped_values: float32 [64, 262144], P('bump', ('nx', 'ny'))
- vega: float32 [64], P('bump')
The draws below stay inside these ranges and needn't reach their ends.
Inputs may be any that keep to these rules, and one draw needn't show every extreme that they name: `tables`: component 0 lies in [0.9, 1], components 1 and 3 in [0.1, 0.2], components 2 and 4 in [0.02, 0.06].
All inputs are finite; a program needn't handle non-finite values.
Results may differ from the reference program's by a relative error of at most 0.0003.
Values sent between devices are 32-bit elements; how exact they have to be, the bound alone decides.
A program may use at most 64 MiB of HBM per device.

```python
import math
import jax
import jax.numpy as jnp
from jax import lax

STEPS = 8
BLOCK = 256
NODES = 262144
BUMPS = 64


def draw_tables(key, part):
    lower = jnp.array([0.9, 0.1, 0.02, 0.1, 0.02], jnp.float32)
    upper = jnp.array([1.0, 0.2, 0.06, 0.2, 0.06], jnp.float32)
    unit = jax.random.uniform(key, (STEPS, 5, NODES), jnp.float32)
    return lower[None, :, None] + (upper - lower)[None, :, None] * unit


def draw_positions(key, part):
    ramp = jnp.exp(jnp.log(3.0) * jnp.arange(NODES, dtype=jnp.float32) / NODES)
    noise = jax.random.normal(key, (NODES,), jnp.float32)
    return jnp.clip(noise * ramp, -6.0, 6.0) * 2.0


def set_ends(values, own_key, least, largest):
    place = [jax.random.randint(jax.random.fold_in(own_key, axis), (), 0, length) for axis, length in enumerate(values.shape)]
    main_axis = values.shape.index(max(values.shape))
    next_to = place[:main_axis] + [(place[main_axis] + 1) % values.shape[main_axis]] + place[main_axis + 1:]
    return values.at[tuple(place)].set(least).at[tuple(next_to)].set(largest)


def block_levels(rng, shape, cuts, least, top_value):
    loudness, own = 1.0, jax.random.fold_in(rng, 6)
    for axis_at, parts in cuts:
        steps = jnp.exp(jax.random.uniform(jax.random.fold_in(own, axis_at), (parts,), jnp.float32, least / len(cuts), top_value / len(cuts)))
        loudness = loudness * jnp.repeat(steps, shape[axis_at] // parts).reshape([-1 if axis == axis_at else 1 for axis in range(len(shape))])
    return loudness


def gaussian(rng, dims, deviation, most, pieces=(), kind=jnp.bfloat16):
    gain = block_levels(rng, dims, pieces, -0.22, 0.18) if pieces else 1.0
    values = jax.random.normal(rng, dims, jnp.float32) * deviation * gain
    return jnp.minimum(jnp.maximum(values, -most), most).astype(kind)


def setup_inputs(seed: int = 0) -> dict:
    key_of = jax.random.split(jax.random.key(seed), 8)
    payoff = gaussian(key_of[0], (NODES,), 1.0, 6.0, ((0, 8),), jnp.float32)
    positions = draw_positions(jax.random.fold_in(key_of[7], 71), 0)
    tables = draw_tables(jax.random.fold_in(key_of[7], 71), 0)
    offsets = set_ends(jax.random.randint(key_of[3], (STEPS, NODES // BLOCK), -1, 2), jax.random.fold_in(key_of[3], 1), -1, 1).astype(jnp.int32)
    vol_curve = jnp.clip(jnp.exp(jax.random.uniform(key_of[4], (STEPS,), jnp.float32, math.log(0.5), math.log(1.2))), 0.5, 1.2)
    bucket = set_ends(jax.random.randint(key_of[5], (BUMPS,), 0, STEPS), jax.random.fold_in(key_of[5], 1), 0, STEPS - 1).astype(jnp.int32)
    bump_size = jnp.clip(jnp.exp(math.log(0.4) - 1.3862944 * jax.random.uniform(key_of[6], (BUMPS,), jnp.float32) ** block_levels(key_of[6], (BUMPS,), ((0, 4),), -0.2, 0.2)), 0.1, 0.4)
    return dict(payoff=payoff, positions=positions, tables=tables, offsets=offsets, vol_curve=vol_curve, bucket=bucket, bump_size=bump_size)


def advance(padded, table, branch_nodes, variance):
    count = padded.shape[-1] - 4

    def shifted(shift_by):
        return padded[..., 2 + shift_by:2 + shift_by + count]

    upward = table[1] + variance * table[2]
    downward = table[3] + variance * table[4]
    middle = 1.0 - upward - downward
    low_case = upward * shifted(0) + middle * shifted(-1) + downward * shifted(-2)
    even_case = upward * shifted(1) + middle * shifted(0) + downward * shifted(-1)
    high_case = upward * shifted(2) + middle * shifted(1) + downward * shifted(0)
    mixed = jnp.where(branch_nodes == -1, low_case, jnp.where(branch_nodes == 0, even_case, high_case))
    return table[0] * mixed


def reference(payoff, positions, tables, offsets, vol_curve, bucket, bump_size):
    block_len = NODES // offsets.shape[1]

    def rollback(variance_row):
        values = payoff
        for step in reversed(range(STEPS)):
            padded = jnp.pad(values, 2, mode="wrap")
            branch_nodes = jnp.repeat(offsets[step], block_len)
            values = advance(padded, tables[step], branch_nodes, variance_row[step])
        return values

    base_values = rollback(vol_curve * vol_curve)
    step_ids = jnp.arange(STEPS, dtype=jnp.int32)
    sigma_rows = vol_curve[None, :] + bump_size[:, None] * (bucket[:, None] == step_ids[None, :]).astype(jnp.float32)

    def one_curve(variance_row):
        values = rollback(variance_row)
        return values, jnp.sum(positions * (values - base_values))

    bumped_values, weighted = lax.map(one_curve, sigma_rows * sigma_rows)
    return bumped_values, weighted / bump_size
```

```python
import functools

import jax
import jax.numpy as jnp
from jax import lax
from jax.experimental import pallas as pl
from jax.experimental.pallas import tpu as pltpu
from jax.sharding import PartitionSpec as P

LANES = 128
SUB = 8
VMEM_LIMIT = 24 * 1024 * 1024
MESH = pl.DeviceIdType.MESH


def sweep_kernel(
    dims,
    vol_ref,
    payoff_ref,
    positions_ref,
    offsets_ref,
    tables_ref,
    rows_ref,
    sums_ref,
    tab,
    pay,
    offs,
    kmask,
    state,
    part,
    part2,
    tab_send,
    tab_recv,
    nb_send,
    nb_recv,
    own_sem,
    res_send,
    res_recv,
    ring_send,
    ring_recv,
    grp_send,
    grp_recv,
):
    n, nx, ny, steps, per, block_len, chunks = dims
    ring_size = nx * ny
    rows = payoff_ref.shape[0]
    quarter = rows // n
    ext = quarter + 2 * SUB
    span = quarter // chunks
    wide = span + 2 * SUB
    me = lax.axis_index("bump")
    ring = lax.axis_index("nx") * ny + lax.axis_index("ny")

    def at(r, q):
        return {"bump": q, "nx": r // ny, "ny": r % ny}

    right = lax.rem(ring + 1, ring_size)
    left = lax.rem(ring + ring_size - 1, ring_size)

    barrier = pltpu.get_barrier_semaphore()
    peers = [at(ring, lax.rem(me + i, n)) for i in range(1, n)]
    peers += [at(lax.rem(ring + i, ring_size), me) for i in range(1, ring_size)]
    peers += [at(r, lax.rem(me + i, n)) for i in range(1, n) for r in (left, right)]
    for peer in peers:
        pl.semaphore_signal(barrier, inc=1, device_id=peer, device_id_type=MESH)
    pl.semaphore_wait(barrier, len(peers))

    def neighbour(i, src, dst, to):
        return pltpu.make_async_remote_copy(
            src_ref=src,
            dst_ref=dst,
            send_sem=nb_send.at[i],
            recv_sem=nb_recv.at[i],
            device_id=at(to, me),
            device_id_type=MESH,
        )

    near = [
        neighbour(0, payoff_ref.at[rows - SUB : rows], pay.at[0:SUB], right),
        neighbour(1, payoff_ref.at[0:SUB], pay.at[SUB + rows : SUB + rows + SUB], left),
        neighbour(2, offsets_ref, offs.at[0], right),
        neighbour(3, offsets_ref, offs.at[1], left),
    ]
    for copy in near:
        copy.start()

    last = chunks + 1

    def piece(kind, q):
        if kind == 0:
            source = slice((q + 1) * quarter - 1, (q + 1) * quarter)
            target = (q + 1) % n
            return target, (right if q == n - 1 else ring), source, slice(SUB - 1, SUB)
        if kind == last:
            source = slice(q * quarter, q * quarter + 1)
            target = (q - 1) % n
            landing = slice(SUB + quarter, SUB + quarter + 1)
            return target, (left if q == 0 else ring), source, landing
        lo = 0 if kind == 1 else (kind - 1) * span + SUB
        hi = quarter if kind == chunks else kind * span + SUB
        source = slice(q * quarter + lo, q * quarter + hi)
        return q, ring, source, slice(SUB + lo, SUB + hi)

    def table_copy(kind, q):
        target, at_ring, source, landing = piece(kind, q)
        crosses = (kind == 0 and q == n - 1) or (kind == last and q == 0)
        src = tables_ref.at[:, source]
        dst = tab.at[me, :, landing]

        def remote():
            return pltpu.make_async_remote_copy(
                src_ref=src,
                dst_ref=dst,
                send_sem=tab_send.at[kind, q],
                recv_sem=tab_recv.at[kind, me],
                device_id=at(at_ring, target),
                device_id_type=MESH,
            )

        def local():
            return pltpu.make_async_copy(src, dst, tab_recv.at[kind, me])

        return target, crosses, remote, local

    for kind in range(last + 1):
        for q in range(n):
            target, crosses, remote, local = table_copy(kind, q)
            if crosses:
                remote().start()
            else:
                pl.when(me != target)(lambda: remote().start())
                pl.when(me == target)(lambda: local().start())

    own = pltpu.make_async_copy(payoff_ref, pay.at[SUB : SUB + rows], own_sem)
    own.start()
    for copy in near:
        copy.wait()
    own.wait()

    blocks = offsets_ref.shape[1]
    rows_per_block = block_len // LANES
    row_at = lax.broadcasted_iota(jnp.int32, (ext, blocks), 0) + me * quarter
    row_at = row_at + (rows - SUB)
    block_at = row_at // rows_per_block - blocks
    lane_at = lax.broadcasted_iota(jnp.int32, (ext, blocks), 1)
    for s in range(steps):
        def spread(line, shift):
            hit = lane_at == block_at + shift
            return jnp.where(hit, line.astype(jnp.float32), 0.0)

        picked = (
            spread(offsets_ref[s : s + 1, :], 0)
            + spread(offs[0, s : s + 1, :], blocks)
            + spread(offs[1, s : s + 1, :], -blocks)
        )
        branch = jnp.sum(picked, axis=1, keepdims=True)
        kmask[s] = jnp.broadcast_to(branch, (ext, LANES))

    lane = lax.broadcasted_iota(jnp.int32, (wide, LANES), 1)

    def waits(kind, src):
        _, _, source, landing = piece(kind, 0)
        dst = tab.at[src, :, landing]
        pltpu.make_async_copy(tables_ref.at[:, source], dst, tab_recv.at[kind, src]).wait()

    def shifts(x):
        f1 = pltpu.roll(x, LANES - 1, 1)
        f2 = pltpu.roll(x, LANES - 2, 1)
        b1 = pltpu.roll(x, 1, 1)
        b2 = pltpu.roll(x, 2, 1)
        f1 = jnp.where(lane >= LANES - 1, pltpu.roll(f1, wide - 1, 0), f1)
        f2 = jnp.where(lane >= LANES - 2, pltpu.roll(f2, wide - 1, 0), f2)
        b1 = jnp.where(lane < 1, pltpu.roll(b1, 1, 0), b1)
        b2 = jnp.where(lane < 2, pltpu.roll(b2, 1, 0), b2)
        return b2, b1, f1, f2

    def roll_back(h):
        window = slice(h * span, h * span + wide)
        state[0] = pay[pl.ds(pl.multiple_of(me * quarter + h * span, SUB), wide), :]
        for s in reversed(range(steps)):
            src, step = s // per, s % per
            if step == per - 1:
                if h == 0:
                    waits(0, src)
                waits(h + 1, src)
                if h == chunks - 1:
                    waits(last, src)
            w = vol_ref[s] * vol_ref[s]
            discount = tab[src, 0, window, step, :]
            slope_up = discount * tab[src, 2, window, step, :]
            slope_down = discount * tab[src, 4, window, step, :]
            up = discount * tab[src, 1, window, step, :] + w * slope_up
            down = discount * tab[src, 3, window, step, :] + w * slope_down
            middle = discount - up - down
            branch = kmask[s, window]
            low = branch < -0.5
            high = branch > 0.5
            for g in [0] + list(range(s + 2, steps + 1)):
                x = state[g]
                b2, b1, f1, f2 = shifts(x)
                above = jnp.where(low, x, jnp.where(high, f2, f1))
                level = jnp.where(low, b1, jnp.where(high, f1, x))
                below = jnp.where(low, b2, jnp.where(high, x, b1))
                state[g] = up * above + middle * level + down * below
                if g == 0:
                    state[s + 1] = slope_up * (above - level) + slope_down * (below - level)
        here = pl.ds(pl.multiple_of(me * quarter + h * span, SUB), span)
        weights = positions_ref[here, :]
        for g in range(steps + 1):
            center = state[g, SUB : SUB + span, :]
            rows_ref[g, here, :] = center
            if g:
                weighted = jnp.sum(weights * center, axis=0, keepdims=True)
                if h:
                    weighted = weighted + part2[me, g - 1 : g, :]
                part2[me, g - 1 : g, :] = weighted

    def result(m, d, slot, h):
        first = jnp.bitwise_xor(me, m) * quarter + h * span
        held = pl.ds(pl.multiple_of(first, SUB), span)
        return pltpu.make_async_remote_copy(
            src_ref=rows_ref.at[:, held, :],
            dst_ref=rows_ref.at[:, held, :],
            send_sem=res_send.at[slot, h],
            recv_sem=res_recv.at[slot, h],
            device_id=at(ring, jnp.bitwise_xor(me, d)),
            device_id_type=MESH,
        )

    plan = []
    masks = [0]
    d = n // 2
    while d:
        plan += [(m, d) for m in masks]
        masks = masks + [m | d for m in masks]
        d //= 2
    slots = {m | d: i for i, (m, d) in enumerate(plan)}
    landed = set()
    copies = [[result(m, d, i, h) for h in range(chunks)] for i, (m, d) in enumerate(plan)]
    grp_copies = []
    for i in range(1, n):
        grp_copies.append(
            pltpu.make_async_remote_copy(
                src_ref=part2.at[me],
                dst_ref=part2.at[me],
                send_sem=grp_send.at[i],
                recv_sem=grp_recv.at[i],
                device_id=at(ring, lax.rem(me + i, n)),
                device_id_type=MESH,
            )
        )
    ring_copies = []
    for i in range(1, ring_size):
        ring_copies.append(
            pltpu.make_async_remote_copy(
                src_ref=part.at[ring],
                dst_ref=part.at[ring],
                send_sem=ring_send.at[i],
                recv_sem=ring_recv.at[i],
                device_id=at(lax.rem(ring + i, ring_size), me),
                device_id_type=MESH,
            )
        )

    def forward(h):
        for i, (m, d) in enumerate(plan):
            if m != 0:
                if (m, h) not in landed:
                    landed.add((m, h))
                    copies[slots[m]][h].wait_recv()
                copies[i][h].start()

    for h in range(chunks):
        roll_back(h)
        if h == chunks - 1:
            for copy in grp_copies:
                copy.start()
        for i, (m, d) in enumerate(plan):
            if m == 0:
                copies[i][h].start()
    for i in range(1, n):
        src = lax.rem(me + n - i, n)
        pltpu.make_async_copy(part2.at[src], part2.at[src], grp_recv.at[i]).wait()
    part[ring] = jnp.sum(part2[...], axis=0)
    for copy in ring_copies:
        copy.start()
    for h in range(chunks):
        forward(h)
    for i in range(1, ring_size):
        src = lax.rem(ring + ring_size - i, ring_size)
        pltpu.make_async_copy(part.at[src], part.at[src], ring_recv.at[i]).wait()
    sums_ref[...] = jnp.sum(part[...], axis=0)
    for copy in grp_copies + ring_copies:
        copy.wait_send()
    for h in range(chunks):
        for i, (m, d) in enumerate(plan):
            copies[i][h].wait_send()
            if (m | d, h) not in landed:
                copies[i][h].wait_recv()
    for kind in range(last + 1):
        for q in range(n):
            target, crosses, remote, _ = table_copy(kind, q)
            if crosses:
                remote().wait_send()
            else:
                pl.when(me != target)(lambda: remote().wait_send())


def spread_kernel(vol_ref, bucket_ref, bump_ref, rows_ref, sums_ref, out_ref, vega_ref, held, sem):
    curves = bucket_ref.shape[0]
    rows = rows_ref.shape[1]
    parts = sem.shape[0]
    span = rows // parts
    picks = []
    for b in range(curves):
        s = bucket_ref[b]
        slope = 2.0 * vol_ref[s] + bump_ref[b]
        picks.append((s, slope, bump_ref[b] * slope))
    copies = []
    for i in range(parts):
        here = slice(i * span, (i + 1) * span)
        base = rows_ref[0, here, :]
        for b in range(curves):
            s, _, change = picks[b]
            held[b // SUB, here, b % SUB, :] = base + change * rows_ref[s + 1, here, :]
        copy = pltpu.make_async_copy(held.at[:, here], out_ref.at[:, here], sem.at[i])
        copy.start()
        copies.append(copy)
    lane = lax.broadcasted_iota(jnp.int32, (1, curves), 1)
    total = jnp.zeros((1, curves), jnp.float32)
    for b in range(curves):
        s, slope, _ = picks[b]
        weighted = jnp.sum(sums_ref[pl.ds(s, 1), :], axis=1, keepdims=True)
        total = jnp.where(lane == b, slope * weighted, total)
    vega_ref[...] = total
    for copy in copies:
        copy.wait()


def on_device(n, nx, ny, payoff, positions, tables, offsets, vol_curve, bucket, bump_size):
    steps = vol_curve.shape[0]
    per, comps, nodes = tables.shape
    curves = bucket.shape[0]
    rows = nodes // LANES
    block_len = nodes // offsets.shape[1]
    quarter = rows // n
    ext = quarter + 2 * SUB
    ring = nx * ny
    chunks = 2
    wide = quarter // chunks + 2 * SUB
    tiles = tables.transpose(1, 0, 2).reshape(comps, per, rows, LANES).transpose(0, 2, 1, 3)
    dma = pltpu.SemaphoreType.DMA
    vmem = pl.BlockSpec(memory_space=pltpu.VMEM)
    smem = pl.BlockSpec(memory_space=pltpu.SMEM)
    moved, sums = pl.pallas_call(
        functools.partial(sweep_kernel, (n, nx, ny, steps, per, block_len, chunks)),
        out_shape=(
            pltpu.VMEM((steps + 1, rows, LANES), jnp.float32),
            pltpu.VMEM((steps, LANES), jnp.float32),
        ),
        in_specs=[smem, vmem, vmem, vmem, pl.BlockSpec(memory_space=pl.ANY)],
        out_specs=(vmem, vmem),
        scratch_shapes=[
            pltpu.VMEM((n, comps, ext, per, LANES), jnp.float32),
            pltpu.VMEM((rows + 2 * SUB, LANES), jnp.float32),
            pltpu.VMEM((2,) + offsets.shape, jnp.int32),
            pltpu.VMEM((steps, ext, LANES), jnp.float32),
            pltpu.VMEM((steps + 1, wide, LANES), jnp.float32),
            pltpu.VMEM((ring, steps, LANES), jnp.float32),
            pltpu.VMEM((n, steps, LANES), jnp.float32),
            dma((chunks + 2, n)),
            dma((chunks + 2, n)),
            dma((4,)),
            dma((4,)),
            dma,
            dma((n - 1, chunks)),
            dma((n - 1, chunks)),
            dma((ring,)),
            dma((ring,)),
            dma((n,)),
            dma((n,)),
        ],
        compiler_params=pltpu.CompilerParams(
            has_side_effects=True, collective_id=0, vmem_limit_bytes=VMEM_LIMIT
        ),
        name="sweep",
    )(
        *[
            pltpu.with_memory_space_constraint(x, pltpu.HBM)
            for x in (
                vol_curve,
                payoff.reshape(rows, LANES),
                positions.reshape(rows, LANES),
                offsets,
                tiles,
            )
        ]
    )
    groups = curves // SUB
    parts = max(1, rows // (4 * SUB))
    bumped, vega = pl.pallas_call(
        spread_kernel,
        out_shape=(
            jax.ShapeDtypeStruct((groups, rows, SUB, LANES), jnp.float32),
            jax.ShapeDtypeStruct((1, curves), jnp.float32),
        ),
        in_specs=[smem, smem, smem, vmem, vmem],
        out_specs=(pl.BlockSpec(memory_space=pl.ANY), vmem),
        scratch_shapes=[pltpu.VMEM((groups, rows, SUB, LANES), jnp.float32), dma((parts,))],
        compiler_params=pltpu.CompilerParams(vmem_limit_bytes=VMEM_LIMIT),
        name="spread",
    )(
        *[pltpu.with_memory_space_constraint(x, pltpu.HBM) for x in (vol_curve, bucket, bump_size)],
        moved,
        sums,
    )
    bumped = bumped.transpose(0, 2, 1, 3).reshape(curves, nodes)
    return bumped, vega.reshape(curves)


def solution(mesh):
    shape = dict(mesh.shape)
    in_specs = (
        P(("nx", "ny")),
        P(("nx", "ny")),
        P("bump", None, ("nx", "ny")),
        P(None, ("nx", "ny")),
        P(),
        P("bump"),
        P("bump"),
    )
    out_specs = (P("bump", ("nx", "ny")), P("bump"))
    body = functools.partial(on_device, shape["bump"], shape["nx"], shape["ny"])
    return jax.shard_map(body, mesh=mesh, in_specs=in_specs, out_specs=out_specs, check_vma=False)
```

```python
import functools

import jax
import jax.numpy as jnp
from jax import lax
from jax.experimental import pallas as pl
from jax.experimental.pallas import tpu as pltpu
from jax.sharding import PartitionSpec as P

LANES = 128
SUB = 8
VMEM_LIMIT = 24 * 1024 * 1024
MESH = pl.DeviceIdType.MESH


def sweep_kernel(
    dims,
    vol_ref,
    payoff_ref,
    positions_ref,
    offsets_ref,
    tables_ref,
    rows_ref,
    sums_ref,
    tab,
    pay,
    pos,
    offs,
    coef,
    state,
    mid,
    part,
    tot,
    loc_sem,
    tab_send,
    tab_recv,
    halo_send,
    halo_recv,
    mid_send,
    mid_recv,
    far_send,
    far_recv,
    near_send,
    near_recv,
    ring_send,
    ring_recv,
    tot_send,
    tot_recv,
):
    n, nx, ny, steps, per, block_len, bounds = dims
    ring_size = nx * ny
    rows = payoff_ref.shape[0]
    blocks = offsets_ref.shape[1]
    group = n // 2
    half = steps // 2
    share = rows // group
    chunks = len(bounds) - 1
    me = lax.axis_index("bump")
    ring = lax.axis_index("nx") * ny + lax.axis_index("ny")
    side = me // group
    core = lax.rem(me, group)
    upper = side == 1
    lower = side == 0
    first = core == 0

    def at(r, q):
        return {"bump": q, "nx": r // ny, "ny": lax.rem(r, ny)}

    right = lax.rem(ring + 1, ring_size)
    left = lax.rem(ring + ring_size - 1, ring_size)
    sibling = at(ring, side * group + (1 - core))
    across = at(ring, (1 - side) * group + core)
    diagonal = at(ring, (1 - side) * group + (1 - core))
    outer = at(jnp.where(first, right, left), me)

    def start_of(c, a, b):
        return pl.multiple_of(SUB + jnp.where(c == 0, share - b, a), SUB)

    def local(a, b):
        return pl.ds(start_of(core, a, b), b - a)

    def wide_at(c, a, b):
        return pl.ds(pl.multiple_of(start_of(c, a, b) + c * share, SUB), b - a)

    def owned_at(c, a, b):
        return pl.ds(pl.multiple_of(start_of(c, a, b) + c * share - SUB, SUB), b - a)

    def table_at(c, a, b):
        begin = (start_of(c, a, b) + c * share) * per
        return pl.ds(pl.multiple_of(begin, SUB * per), (b - a) * per)

    whole = slice(SUB * per, (SUB + rows) * per)
    loads = [
        pltpu.make_async_copy(tables_ref, tab.at[core, :, whole], loc_sem.at[0]),
        pltpu.make_async_copy(payoff_ref, pay.at[SUB : SUB + rows], loc_sem.at[1]),
        pltpu.make_async_copy(positions_ref, pos, loc_sem.at[2]),
        pltpu.make_async_copy(offsets_ref, offs.at[0], loc_sem.at[3]),
    ]
    for copy in loads:
        copy.start()

    barrier = pltpu.get_barrier_semaphore()
    peers = [at(ring, lax.rem(me + i, n)) for i in range(1, n)]
    peers += [at(lax.rem(ring + i, ring_size), me) for i in range(1, ring_size)]
    for peer in peers:
        pl.semaphore_signal(barrier, inc=1, device_id=peer, device_id_type=MESH)
    for copy in loads:
        copy.wait()
    pl.semaphore_wait(barrier, len(peers))

    def remote(src, dst, send, recv, to):
        return pltpu.make_async_remote_copy(
            src_ref=src, dst_ref=dst, send_sem=send, recv_sem=recv, device_id=to, device_id_type=MESH
        )

    def fresh(j):
        lo = -SUB if j == 0 else min(bounds[j] + 2 * SUB, share)
        return lo, min(bounds[j + 1] + 2 * SUB, share)

    table_copies = []
    pieces = [fresh(j) for j in range(chunks)]
    for j, (lo, hi) in enumerate(pieces):
        there = tab.at[core, :, table_at(1 - core, lo, hi)]
        table_copies.append(remote(there, there, tab_send.at[j], tab_recv.at[j], sibling))
    there = tab.at[core, :, table_at(1 - core, share - SUB, share)]
    edge = pl.multiple_of(jnp.where(first, SUB, rows) * per, SUB * per)
    there = tab.at[core, :, pl.ds(edge, SUB * per)]
    table_copies.append(remote(there, there, tab_send.at[chunks], tab_recv.at[chunks], sibling))
    order = [0, chunks] + list(range(1, chunks))
    for j in order:
        table_copies[j].start()

    def arrived(j):
        lo, hi = pieces[j]
        here = tab.at[1 - core, :, table_at(core, lo, hi)]
        return remote(here, here, tab_send.at[j], tab_recv.at[j], sibling)

    out_from = pl.multiple_of(jnp.where(first, rows, SUB), SUB)
    out_to = pl.multiple_of(jnp.where(first, 0, rows + SUB), SUB)
    out_tab = pl.ds(pl.multiple_of(out_from * per, SUB * per), SUB * per)
    in_tab = pl.ds(pl.multiple_of(out_to * per, SUB * per), SUB * per)
    halo_copies = [
        remote(
            pay.at[pl.ds(out_from, SUB)], pay.at[pl.ds(out_to, SUB)],
            halo_send.at[0], halo_recv.at[0], outer,
        ),
        remote(offs.at[0], offs.at[1], halo_send.at[1], halo_recv.at[1], outer),
        remote(tab.at[:, :, out_tab], tab.at[:, :, in_tab], halo_send.at[2], halo_recv.at[2], outer),
    ]
    halo_copies[0].start()
    halo_copies[1].start()

    def send_tables_out():
        mine = remote(
            tab.at[1 - core, :, out_tab], tab.at[1 - core, :, out_tab],
            tab_send.at[chunks], tab_recv.at[chunks], sibling,
        )
        mine.wait_recv()
        halo_copies[2].start()

    def prepare(a, b, source):
        count = b - a
        begin = start_of(core, a, b)
        row = lax.broadcasted_iota(jnp.int32, (count, blocks), 0) + (begin - SUB + core * share + rows)
        hit = lax.broadcasted_iota(jnp.int32, (count, blocks), 1) == lax.rem(row, rows) * LANES // block_len
        here = pl.ds(begin, count)
        for t in range(half):
            step = side * half + t
            slot, at_step = t // per, t % per
            line = offs[source, pl.ds(step, 1), :].astype(jnp.float32)
            branch = jnp.sum(jnp.where(hit, line, 0.0), axis=1, keepdims=True)
            branch = jnp.broadcast_to(branch, (count, LANES))
            low = branch < -0.5
            high = branch > 0.5

            def entry(k):
                first_row = (begin + core * share) * per + at_step
                return tab[slot, k, pl.ds(first_row, count, stride=per), :]

            w = vol_ref[step] * vol_ref[step]
            discount = entry(0)
            slope_up = discount * entry(2)
            slope_down = discount * entry(4)
            up = discount * entry(1) + w * slope_up
            down = discount * entry(3) + w * slope_down
            middle = discount - up - down
            slope_mid = -slope_up - slope_down

            def put(k, above, level, below):
                zero = jnp.zeros_like(above)
                coef[t, k, here, :] = jnp.where(high, above, zero)
                coef[t, k + 1, here, :] = jnp.where(high, level, jnp.where(low, zero, above))
                coef[t, k + 2, here, :] = jnp.where(high, below, jnp.where(low, above, level))
                coef[t, k + 3, here, :] = jnp.where(high, zero, jnp.where(low, level, below))
                coef[t, k + 4, here, :] = jnp.where(low, below, zero)

            put(0, up, middle, down)
            put(5, slope_up, slope_mid, slope_down)

    def advance(a, b, top):
        count = b - a
        here = local(a, b)
        lane = lax.broadcasted_iota(jnp.int32, (count, LANES), 1)
        for t in reversed(range(half)):
            s = top + t
            c = [coef[t, k, here, :] for k in range(5)]
            for g in [0] + list(range(s + 2, steps + 1)):
                x = state[g, 0:count, :]
                after = pltpu.roll(x, count - 1, 0)
                before = pltpu.roll(x, 1, 0)
                f1 = pltpu.roll(jnp.where(lane < 1, after, x), LANES - 1, 1)
                f2 = pltpu.roll(jnp.where(lane < 2, after, x), LANES - 2, 1)
                b1 = pltpu.roll(jnp.where(lane >= LANES - 1, before, x), 1, 1)
                b2 = pltpu.roll(jnp.where(lane >= LANES - 2, before, x), 2, 1)
                state[g, 0:count, :] = c[0] * f2 + c[1] * f1 + c[2] * x + c[3] * b1 + c[4] * b2
                if g == 0:
                    e = [coef[t, 5 + k, here, :] for k in range(5)]
                    state[s + 1, 0:count, :] = e[0] * f2 + e[1] * f1 + e[2] * x + e[3] * b1 + e[4] * b2

    passed = [0] + list(range(half + 1, steps + 1))

    def mid_piece(j):
        return (-SUB if j == 0 else bounds[j] + SUB), bounds[j + 1] + SUB

    def mid_copy(j):
        lo, hi = mid_piece(j)
        here = mid.at[:, local(lo, hi)]
        return remote(here, here, mid_send.at[j], mid_recv.at[j], across)

    def result_at(c, j):
        return rows_ref.at[:, owned_at(c, bounds[j], bounds[j + 1])]

    def far_copy(j):
        here = result_at(core, j)
        return remote(here, here, far_send.at[j], far_recv.at[j], across)

    def near_copy(j):
        here = result_at(core, j)
        return remote(here, here, near_send.at[j], near_recv.at[j], sibling)

    def near_landed(j):
        here = result_at(1 - core, j)
        return remote(here, here, near_send.at[j], near_recv.at[j], sibling)

    @pl.when(upper)
    def _():
        for j in range(chunks):
            lo, hi = mid_piece(j)
            begin, end = max(lo - SUB, -SUB), min(hi + SUB, share + SUB)
            arrived(j).wait_recv()
            if j == 0:
                prepare(*pieces[0], 0)
                send_tables_out()
            elif pieces[j][0] < pieces[j][1]:
                prepare(*pieces[j], 0)
            if j == chunks - 1:
                for copy in halo_copies:
                    copy.wait_recv()
                prepare(share, share + SUB, 1)
            count = end - begin
            state[0, 0:count, :] = pay[wide_at(core, begin, end), :]
            advance(begin, end, half)
            shift = pl.multiple_of(jnp.where(first, end - hi, lo - begin), SUB)
            for i, g in enumerate(passed):
                mid[i, local(lo, hi), :] = state[g, pl.ds(shift, hi - lo), :]
            mid_copy(j).start()
        for j in range(chunks):
            far_copy(j).wait_recv()
            near_copy(j).start()
        for c in range(group):
            total = tot.at[c]
            remote(total, total, tot_send.at[c], tot_recv.at[c], across).wait_recv()
        for j in range(chunks):
            mid_copy(j).wait_send()

    @pl.when(lower)
    def _():
        for j in range(chunks):
            arrived(j).wait_recv()
            if j == 0:
                send_tables_out()
            if pieces[j][0] < pieces[j][1]:
                prepare(*pieces[j], 0)
        for j in range(chunks):
            lo, hi = bounds[j], bounds[j + 1]
            begin, end = lo - SUB, hi + SUB
            if j == chunks - 1:
                for copy in halo_copies:
                    copy.wait_recv()
                prepare(share, share + SUB, 1)
            mid_copy(j).wait_recv()
            count = end - begin
            for i, g in enumerate(passed):
                state[g, 0:count, :] = mid[i, local(begin, end), :]
            advance(begin, end, 0)
            here = owned_at(core, lo, hi)
            weights = pos[here, :]
            for g in range(steps + 1):
                center = state[g, SUB : SUB + hi - lo, :]
                rows_ref[g, here, :] = center
                if g:
                    weighted = jnp.sum(weights * center, axis=0, keepdims=True)
                    if j:
                        weighted = weighted + part[ring, g - 1 : g, :]
                    part[ring, g - 1 : g, :] = weighted
            far_copy(j).start()
            near_copy(j).start()
        ring_copies = []
        for i in range(1, ring_size):
            mine = part.at[ring]
            to = at(lax.rem(ring + i, ring_size), me)
            ring_copies.append(remote(mine, mine, ring_send.at[i], ring_recv.at[i], to))
        for copy in ring_copies:
            copy.start()
        for i in range(1, ring_size):
            other = part.at[lax.rem(ring + ring_size - i, ring_size)]
            remote(other, other, ring_send.at[i], ring_recv.at[i], sibling).wait_recv()
        tot[core] = jnp.sum(part[...], axis=0)
        total = tot.at[core]
        tot_copies = [
            remote(total, total, tot_send.at[i], tot_recv.at[core], to)
            for i, to in enumerate((sibling, across, diagonal))
        ]
        for copy in tot_copies:
            copy.start()
        other = tot.at[1 - core]
        remote(other, other, tot_send.at[0], tot_recv.at[1 - core], sibling).wait_recv()
        for copy in ring_copies + tot_copies:
            copy.wait_send()
        for j in range(chunks):
            far_copy(j).wait_send()

    sums_ref[...] = jnp.sum(tot[...], axis=0)
    for j in range(chunks):
        near_landed(j).wait_recv()
        near_copy(j).wait_send()
    for copy in table_copies + halo_copies:
        copy.wait_send()


def spread_kernel(vol_ref, bucket_ref, bump_ref, rows_ref, sums_ref, out_ref, vega_ref, held, sem):
    curves = bucket_ref.shape[0]
    groups = curves // SUB
    rows = rows_ref.shape[1]
    parts = sem.shape[0]
    span = rows // parts
    picks = []
    for b in range(curves):
        s = bucket_ref[b]
        slope = 2.0 * vol_ref[s] + bump_ref[b]
        picks.append((s, slope, bump_ref[b] * slope))
    copies = []
    for i in range(parts):
        here = slice(i * span, (i + 1) * span)
        base = rows_ref[0, here, :]
        for b in range(curves):
            s, _, change = picks[b]
            line = (b // SUB * rows + i * span) * SUB + b % SUB
            held[pl.ds(line, span, stride=SUB), :] = base + change * rows_ref[s + 1, here, :]
        for g in range(groups):
            place = slice((g * rows + i * span) * SUB, (g * rows + (i + 1) * span) * SUB)
            copy = pltpu.make_async_copy(held.at[place], out_ref.at[place], sem.at[i, g])
            copy.start()
            copies.append(copy)
    lane = lax.broadcasted_iota(jnp.int32, (1, curves), 1)
    total = jnp.zeros((1, curves), jnp.float32)
    for b in range(curves):
        s, slope, _ = picks[b]
        weighted = jnp.sum(sums_ref[pl.ds(s, 1), :], axis=1, keepdims=True)
        total = jnp.where(lane == b, slope * weighted, total)
    vega_ref[...] = total
    for copy in copies:
        copy.wait()


def on_device(n, nx, ny, payoff, positions, tables, offsets, vol_curve, bucket, bump_size):
    steps = vol_curve.shape[0]
    per, comps, nodes = tables.shape
    curves = bucket.shape[0]
    rows = nodes // LANES
    block_len = nodes // offsets.shape[1]
    group = n // 2
    share = rows // group
    half = steps // 2
    ring = nx * ny
    bounds = [share * k // (8 * SUB) * SUB for k in (0, 1, 3, 5, 8)]
    chunks = len(bounds) - 1
    widest = max(b - a for a, b in zip(bounds, bounds[1:])) + 3 * SUB
    tiles = tables.transpose(1, 0, 2).reshape(comps, per, rows, LANES).transpose(0, 2, 1, 3)
    tiles = tiles.reshape(comps, rows * per, LANES)
    dma = pltpu.SemaphoreType.DMA
    vmem = pl.BlockSpec(memory_space=pltpu.VMEM)
    smem = pl.BlockSpec(memory_space=pltpu.SMEM)
    hbm = pl.BlockSpec(memory_space=pltpu.HBM)

    def keep(x):
        return pltpu.with_memory_space_constraint(x, pltpu.HBM)

    moved, sums = pl.pallas_call(
        functools.partial(sweep_kernel, (n, nx, ny, steps, per, block_len, bounds)),
        out_shape=(
            pltpu.VMEM((steps + 1, rows, LANES), jnp.float32),
            pltpu.VMEM((steps, LANES), jnp.float32),
        ),
        in_specs=[smem, hbm, hbm, hbm, hbm],
        out_specs=(vmem, vmem),
        scratch_shapes=[
            pltpu.VMEM((group, comps, (rows + 2 * SUB) * per, LANES), jnp.float32),
            pltpu.VMEM((rows + 2 * SUB, LANES), jnp.float32),
            pltpu.VMEM((rows, LANES), jnp.float32),
            pltpu.VMEM((2,) + offsets.shape, jnp.int32),
            pltpu.VMEM((half, 10, share + 2 * SUB, LANES), jnp.float32),
            pltpu.VMEM((steps + 1, widest, LANES), jnp.float32),
            pltpu.VMEM((half + 1, share + 2 * SUB, LANES), jnp.float32),
            pltpu.VMEM((ring, steps, LANES), jnp.float32),
            pltpu.VMEM((group, steps, LANES), jnp.float32),
            dma((4,)),
            dma((chunks + 1,)),
            dma((chunks + 1,)),
            dma((3,)),
            dma((3,)),
            dma((chunks,)),
            dma((chunks,)),
            dma((chunks,)),
            dma((chunks,)),
            dma((chunks,)),
            dma((chunks,)),
            dma((ring,)),
            dma((ring,)),
            dma((3,)),
            dma((group,)),
        ],
        compiler_params=pltpu.CompilerParams(
            has_side_effects=True, collective_id=0, vmem_limit_bytes=VMEM_LIMIT
        ),
        name="sweep",
    )(
        keep(vol_curve),
        keep(payoff.reshape(rows, LANES)),
        keep(positions.reshape(rows, LANES)),
        keep(offsets),
        keep(tiles),
    )
    groups = curves // SUB
    parts = max(1, rows // (4 * SUB))
    bumped, vega = pl.pallas_call(
        spread_kernel,
        out_shape=(
            jax.ShapeDtypeStruct((groups * rows * SUB, LANES), jnp.float32),
            jax.ShapeDtypeStruct((1, curves), jnp.float32),
        ),
        in_specs=[smem, smem, smem, vmem, vmem],
        out_specs=(pl.BlockSpec(memory_space=pl.ANY), vmem),
        scratch_shapes=[pltpu.VMEM((groups * rows * SUB, LANES), jnp.float32), dma((parts, groups))],
        compiler_params=pltpu.CompilerParams(vmem_limit_bytes=VMEM_LIMIT),
        name="spread",
    )(keep(vol_curve), keep(bucket), keep(bump_size), moved, sums)
    bumped = bumped.reshape(groups, rows, SUB, LANES).transpose(0, 2, 1, 3).reshape(curves, nodes)
    return bumped, vega.reshape(curves)


def solution(mesh):
    shape = dict(mesh.shape)
    in_specs = (
        P(("nx", "ny")),
        P(("nx", "ny")),
        P("bump", None, ("nx", "ny")),
        P(None, ("nx", "ny")),
        P(),
        P("bump"),
        P("bump"),
    )
    out_specs = (P("bump", ("nx", "ny")), P("bump"))
    body = functools.partial(on_device, shape["bump"], shape["nx"], shape["ny"])
    return jax.shard_map(body, mesh=mesh, in_specs=in_specs, out_specs=out_specs, check_vma=False)
```

```python
import functools

import jax
import jax.numpy as jnp
from jax import lax
from jax.experimental import pallas as pl
from jax.experimental.pallas import tpu as pltpu
from jax.sharding import PartitionSpec as P

LANES = 128
SUB = 8
VMEM_LIMIT = 24 * 1024 * 1024
MESH = pl.DeviceIdType.MESH


def sweep_kernel(
    dims,
    vol_ref,
    payoff_ref,
    positions_ref,
    offsets_ref,
    tables_ref,
    rows_ref,
    sums_ref,
    tab,
    pay,
    pos,
    offs,
    coef,
    state,
    mid,
    part,
    tot,
    hello,
    loc_sem,
    tab_send,
    tab_recv,
    halo_send,
    halo_recv,
    mid_send,
    mid_recv,
    far_send,
    far_recv,
    near_send,
    near_recv,
    ring_send,
    ring_recv,
    tot_send,
    tot_recv,
):
    n, nx, ny, steps, per, block_len, bounds = dims
    ring_size = nx * ny
    rows = payoff_ref.shape[0]
    blocks = offsets_ref.shape[1]
    group = n // 2
    half = steps // 2
    share = rows // group
    chunks = len(bounds) - 1
    me = lax.axis_index("bump")
    ring = lax.axis_index("nx") * ny + lax.axis_index("ny")
    side = me // group
    core = lax.rem(me, group)
    upper = side == 1
    lower = side == 0
    first = core == 0

    def at(r, q):
        return {"bump": q, "nx": r // ny, "ny": lax.rem(r, ny)}

    right = lax.rem(ring + 1, ring_size)
    left = lax.rem(ring + ring_size - 1, ring_size)
    sibling = at(ring, side * group + (1 - core))
    across = at(ring, (1 - side) * group + core)
    diagonal = at(ring, (1 - side) * group + (1 - core))
    outer = at(jnp.where(first, right, left), me)

    def start_of(c, a, b):
        return pl.multiple_of(SUB + jnp.where(c == 0, share - b, a), SUB)

    def local(a, b):
        return pl.ds(start_of(core, a, b), b - a)

    def wide_at(c, a, b):
        return pl.ds(pl.multiple_of(start_of(c, a, b) + c * share, SUB), b - a)

    def owned_at(c, a, b):
        return pl.ds(pl.multiple_of(start_of(c, a, b) + c * share - SUB, SUB), b - a)

    def table_at(c, a, b):
        begin = (start_of(c, a, b) + c * share) * per
        return pl.ds(pl.multiple_of(begin, SUB * per), (b - a) * per)

    whole = slice(SUB * per, (SUB + rows) * per)
    loads = [
        pltpu.make_async_copy(tables_ref, tab.at[core, :, whole], loc_sem.at[0]),
        pltpu.make_async_copy(payoff_ref, pay.at[SUB : SUB + rows], loc_sem.at[1]),
        pltpu.make_async_copy(positions_ref, pos, loc_sem.at[2]),
        pltpu.make_async_copy(offsets_ref, offs.at[0], loc_sem.at[3]),
    ]
    for copy in loads:
        copy.start()

    barrier = pltpu.get_barrier_semaphore()

    def greet(sem, to):
        pl.semaphore_signal(sem, inc=1, device_id=to, device_id_type=MESH)

    keeper = jnp.logical_and(lower, first)
    link = jnp.logical_and(upper, first)
    rest = jnp.logical_not(first)

    @pl.when(link)
    def _():
        greet(barrier, sibling)
        greet(barrier, at(left, 0))

    @pl.when(jnp.logical_and(upper, rest))
    def _():
        greet(barrier, at(right, 0))

    @pl.when(lower)
    def _():
        greet(barrier, at(ring, group))
        for i in range(1, ring_size):
            greet(barrier, at(lax.rem(ring + i, ring_size), 0))

    @pl.when(keeper)
    def _():
        greet(barrier, sibling)

    @pl.when(rest)
    def _():
        pl.semaphore_wait(barrier, 1)
        greet(hello.at[0], sibling)

    @pl.when(first)
    def _():
        pl.semaphore_wait(hello.at[0], 1)

    loads[0].wait()

    def remote(src, dst, send, recv, to):
        return pltpu.make_async_remote_copy(
            src_ref=src, dst_ref=dst, send_sem=send, recv_sem=recv, device_id=to, device_id_type=MESH
        )

    def fresh(j):
        lo = -SUB if j == 0 else min(bounds[j] + 2 * SUB, share)
        return lo, min(bounds[j + 1] + 2 * SUB, share)

    table_copies = []
    pieces = [fresh(j) for j in range(chunks)]
    for j, (lo, hi) in enumerate(pieces):
        there = tab.at[core, :, table_at(1 - core, lo, hi)]
        table_copies.append(remote(there, there, tab_send.at[j], tab_recv.at[j], sibling))
    edge = pl.multiple_of(jnp.where(first, SUB, rows) * per, SUB * per)
    there = tab.at[core, :, pl.ds(edge, SUB * per)]
    table_copies.append(remote(there, there, tab_send.at[chunks], tab_recv.at[chunks], sibling))
    order = [j for j, (lo, hi) in enumerate(pieces) if lo < hi] + [chunks]
    for j in order:
        table_copies[j].start()

    def arrived(j):
        lo, hi = pieces[j]
        here = tab.at[1 - core, :, table_at(core, lo, hi)]
        return remote(here, here, tab_send.at[j], tab_recv.at[j], sibling)

    out_from = pl.multiple_of(jnp.where(first, rows, SUB), SUB)
    out_to = pl.multiple_of(jnp.where(first, 0, rows + SUB), SUB)
    out_tab = pl.ds(pl.multiple_of(out_from * per, SUB * per), SUB * per)
    in_tab = pl.ds(pl.multiple_of(out_to * per, SUB * per), SUB * per)
    halo_copies = [
        remote(
            pay.at[pl.ds(out_from, SUB)], pay.at[pl.ds(out_to, SUB)],
            halo_send.at[0], halo_recv.at[0], outer,
        ),
        remote(offs.at[0], offs.at[1], halo_send.at[1], halo_recv.at[1], outer),
        remote(tab.at[:, :, out_tab], tab.at[:, :, in_tab], halo_send.at[2], halo_recv.at[2], outer),
    ]
    landed = remote(
        tab.at[1 - core, :, out_tab], tab.at[1 - core, :, out_tab],
        tab_send.at[chunks], tab_recv.at[chunks], sibling,
    )

    loads[3].wait()

    def prepare(a, b, source):
        count = b - a
        begin = start_of(core, a, b)
        row = lax.broadcasted_iota(jnp.int32, (count, blocks), 0) + (begin - SUB + core * share + rows)
        hit = lax.broadcasted_iota(jnp.int32, (count, blocks), 1) == lax.rem(row, rows) * LANES // block_len
        here = pl.ds(begin, count)
        for t in range(half):
            step = side * half + t
            slot, at_step = t // per, t % per
            line = offs[source, pl.ds(step, 1), :].astype(jnp.float32)
            branch = jnp.sum(jnp.where(hit, line, 0.0), axis=1, keepdims=True)
            branch = jnp.broadcast_to(branch, (count, LANES))
            low = branch < -0.5
            high = branch > 0.5

            def entry(k):
                first_row = (begin + core * share) * per + at_step
                return tab[slot, k, pl.ds(first_row, count, stride=per), :]

            w = vol_ref[step] * vol_ref[step]
            discount = entry(0)
            slope_up = discount * entry(2)
            slope_down = discount * entry(4)
            up = discount * entry(1) + w * slope_up
            down = discount * entry(3) + w * slope_down
            middle = discount - up - down
            slope_mid = -slope_up - slope_down

            def put(k, above, level, below):
                zero = jnp.zeros_like(above)
                coef[t, k, here, :] = jnp.where(high, above, zero)
                coef[t, k + 1, here, :] = jnp.where(high, level, jnp.where(low, zero, above))
                coef[t, k + 2, here, :] = jnp.where(high, below, jnp.where(low, above, level))
                coef[t, k + 3, here, :] = jnp.where(high, zero, jnp.where(low, level, below))
                coef[t, k + 4, here, :] = jnp.where(low, below, zero)

            put(0, up, middle, down)
            put(5, slope_up, slope_mid, slope_down)

    def advance(a, b, top):
        count = b - a
        here = local(a, b)
        lane = lax.broadcasted_iota(jnp.int32, (count, LANES), 1)
        for t in reversed(range(half)):
            s = top + t
            c = [coef[t, k, here, :] for k in range(5)]
            for g in [0] + list(range(s + 2, steps + 1)):
                x = state[g, 0:count, :]
                after = pltpu.roll(x, count - 1, 0)
                before = pltpu.roll(x, 1, 0)
                f1 = pltpu.roll(jnp.where(lane < 1, after, x), LANES - 1, 1)
                f2 = pltpu.roll(jnp.where(lane < 2, after, x), LANES - 2, 1)
                b1 = pltpu.roll(jnp.where(lane >= LANES - 1, before, x), 1, 1)
                b2 = pltpu.roll(jnp.where(lane >= LANES - 2, before, x), 2, 1)
                state[g, 0:count, :] = c[0] * f2 + c[1] * f1 + c[2] * x + c[3] * b1 + c[4] * b2
                if g == 0:
                    e = [coef[t, 5 + k, here, :] for k in range(5)]
                    state[s + 1, 0:count, :] = e[0] * f2 + e[1] * f1 + e[2] * x + e[3] * b1 + e[4] * b2

    passed = [0] + list(range(half + 1, steps + 1))

    def mid_piece(j):
        return (-SUB if j == 0 else bounds[j] + SUB), bounds[j + 1] + SUB

    def mid_copy(j):
        lo, hi = mid_piece(j)
        here = mid.at[:, local(lo, hi)]
        return remote(here, here, mid_send.at[j], mid_recv.at[j], across)

    def result_at(c, j):
        return rows_ref.at[:, owned_at(c, bounds[j], bounds[j + 1])]

    def far_copy(j):
        here = result_at(core, j)
        return remote(here, here, far_send.at[j], far_recv.at[j], across)

    def near_copy(j):
        here = result_at(core, j)
        return remote(here, here, near_send.at[j], near_recv.at[j], sibling)

    def near_landed(j):
        here = result_at(1 - core, j)
        return remote(here, here, near_send.at[j], near_recv.at[j], sibling)

    @pl.when(upper)
    def _():
        loads[1].wait()
        for j in range(chunks):
            lo, hi = mid_piece(j)
            begin, end = max(lo - SUB, -SUB), min(hi + SUB, share + SUB)
            if pieces[j][0] < pieces[j][1]:
                arrived(j).wait_recv()
                prepare(*pieces[j], 0)
            if j == chunks - 1:
                landed.wait_recv()
                pl.semaphore_wait(hello.at[2], 1)
                for copy in halo_copies:
                    copy.start()
                for copy in halo_copies:
                    copy.wait_recv()
                prepare(share, share + SUB, 1)
            count = end - begin
            state[0, 0:count, :] = pay[wide_at(core, begin, end), :]
            advance(begin, end, half)
            shift = pl.multiple_of(jnp.where(first, end - hi, lo - begin), SUB)
            for i, g in enumerate(passed):
                mid[i, local(lo, hi), :] = state[g, pl.ds(shift, hi - lo), :]
            if j == 0:

                @pl.when(first)
                def _():
                    pl.semaphore_wait(barrier, 2)
                    greet(hello.at[1], sibling)

                @pl.when(rest)
                def _():
                    pl.semaphore_wait(hello.at[1], 1)

            mid_copy(j).start()
        for copy in halo_copies:
            copy.wait_send()
        for j in range(chunks):
            far_copy(j).wait_recv()
            near_copy(j).start()
        for c in range(group):
            total = tot.at[c]
            remote(total, total, tot_send.at[c], tot_recv.at[c], across).wait_recv()
        for j in range(chunks):
            mid_copy(j).wait_send()

    @pl.when(lower)
    def _():
        loads[2].wait()
        landed.wait_recv()
        for j in range(chunks):
            if pieces[j][0] < pieces[j][1]:
                arrived(j).wait_recv()
                prepare(*pieces[j], 0)
        for j in range(chunks):
            lo, hi = bounds[j], bounds[j + 1]
            begin, end = lo - SUB, hi + SUB
            if j == 2:

                @pl.when(first)
                def _():
                    pl.semaphore_wait(barrier, 2 * ring_size)
                    greet(hello.at[2], sibling)
                    greet(hello.at[2], across)
                    greet(hello.at[2], diagonal)

                @pl.when(rest)
                def _():
                    pl.semaphore_wait(hello.at[2], 1)

                for copy in halo_copies[1:]:
                    copy.start()
            if j == chunks - 1:
                for copy in halo_copies[1:]:
                    copy.wait_recv()
                prepare(share, share + SUB, 1)
            mid_copy(j).wait_recv()
            count = end - begin
            for i, g in enumerate(passed):
                state[g, 0:count, :] = mid[i, local(begin, end), :]
            advance(begin, end, 0)
            here = owned_at(core, lo, hi)
            weights = pos[here, :]
            for g in range(steps + 1):
                center = state[g, SUB : SUB + hi - lo, :]
                rows_ref[g, here, :] = center
                if g:
                    weighted = jnp.sum(weights * center, axis=0, keepdims=True)
                    if j:
                        weighted = weighted + part[ring, g - 1 : g, :]
                    part[ring, g - 1 : g, :] = weighted
            far_copy(j).start()
            near_copy(j).start()
        ring_copies = []
        for i in range(1, ring_size):
            mine = part.at[ring]
            to = at(lax.rem(ring + i, ring_size), me)
            ring_copies.append(remote(mine, mine, ring_send.at[i], ring_recv.at[i], to))
        for copy in ring_copies:
            copy.start()
        for i in range(1, ring_size):
            other = part.at[lax.rem(ring + ring_size - i, ring_size)]
            remote(other, other, ring_send.at[i], ring_recv.at[i], sibling).wait_recv()
        tot[core] = jnp.sum(part[...], axis=0)
        total = tot.at[core]
        tot_copies = [
            remote(total, total, tot_send.at[i], tot_recv.at[core], to)
            for i, to in enumerate((sibling, across, diagonal))
        ]
        for copy in tot_copies:
            copy.start()
        other = tot.at[1 - core]
        remote(other, other, tot_send.at[0], tot_recv.at[1 - core], sibling).wait_recv()
        for copy in ring_copies + tot_copies + halo_copies[1:]:
            copy.wait_send()
        for j in range(chunks):
            far_copy(j).wait_send()

    sums_ref[...] = jnp.sum(tot[...], axis=0)
    for j in range(chunks):
        near_landed(j).wait_recv()
        near_copy(j).wait_send()
    for j in order:
        table_copies[j].wait_send()

    @pl.when(upper)
    def _():
        loads[2].wait()

    @pl.when(lower)
    def _():
        loads[1].wait()


def spread_kernel(vol_ref, bucket_ref, bump_ref, rows_ref, sums_ref, out_ref, vega_ref, held, sem):
    curves = bucket_ref.shape[0]
    groups = curves // SUB
    rows = rows_ref.shape[1]
    parts = sem.shape[0]
    span = rows // parts
    picks = []
    for b in range(curves):
        s = bucket_ref[b]
        slope = 2.0 * vol_ref[s] + bump_ref[b]
        picks.append((s, slope, bump_ref[b] * slope))
    copies = []
    for i in range(parts):
        here = slice(i * span, (i + 1) * span)
        base = rows_ref[0, here, :]
        for b in range(curves):
            s, _, change = picks[b]
            line = (b // SUB * rows + i * span) * SUB + b % SUB
            held[pl.ds(line, span, stride=SUB), :] = base + change * rows_ref[s + 1, here, :]
        for g in range(groups):
            place = slice((g * rows + i * span) * SUB, (g * rows + (i + 1) * span) * SUB)
            copy = pltpu.make_async_copy(held.at[place], out_ref.at[place], sem.at[i, g])
            copy.start()
            copies.append(copy)
    lane = lax.broadcasted_iota(jnp.int32, (1, curves), 1)
    total = jnp.zeros((1, curves), jnp.float32)
    for b in range(curves):
        s, slope, _ = picks[b]
        weighted = jnp.sum(sums_ref[pl.ds(s, 1), :], axis=1, keepdims=True)
        total = jnp.where(lane == b, slope * weighted, total)
    vega_ref[...] = total
    for copy in copies:
        copy.wait()


def on_device(n, nx, ny, payoff, positions, tables, offsets, vol_curve, bucket, bump_size):
    steps = vol_curve.shape[0]
    per, comps, nodes = tables.shape
    curves = bucket.shape[0]
    rows = nodes // LANES
    block_len = nodes // offsets.shape[1]
    group = n // 2
    share = rows // group
    half = steps // 2
    ring = nx * ny
    bounds = [share * k // (16 * SUB) * SUB for k in (0, 2, 5, 9, 13, 16)]
    chunks = len(bounds) - 1
    widest = max(b - a for a, b in zip(bounds, bounds[1:])) + 3 * SUB
    tiles = tables.transpose(1, 0, 2).reshape(comps, per, rows, LANES).transpose(0, 2, 1, 3)
    tiles = tiles.reshape(comps, rows * per, LANES)
    dma = pltpu.SemaphoreType.DMA
    vmem = pl.BlockSpec(memory_space=pltpu.VMEM)
    smem = pl.BlockSpec(memory_space=pltpu.SMEM)
    hbm = pl.BlockSpec(memory_space=pltpu.HBM)

    def keep(x):
        return pltpu.with_memory_space_constraint(x, pltpu.HBM)

    moved, sums = pl.pallas_call(
        functools.partial(sweep_kernel, (n, nx, ny, steps, per, block_len, bounds)),
        out_shape=(
            pltpu.VMEM((steps + 1, rows, LANES), jnp.float32),
            pltpu.VMEM((steps, LANES), jnp.float32),
        ),
        in_specs=[smem, hbm, hbm, hbm, hbm],
        out_specs=(vmem, vmem),
        scratch_shapes=[
            pltpu.VMEM((group, comps, (rows + 2 * SUB) * per, LANES), jnp.float32),
            pltpu.VMEM((rows + 2 * SUB, LANES), jnp.float32),
            pltpu.VMEM((rows, LANES), jnp.float32),
            pltpu.VMEM((2,) + offsets.shape, jnp.int32),
            pltpu.VMEM((half, 10, share + 2 * SUB, LANES), jnp.float32),
            pltpu.VMEM((steps + 1, widest, LANES), jnp.float32),
            pltpu.VMEM((half + 1, share + 2 * SUB, LANES), jnp.float32),
            pltpu.VMEM((ring, steps, LANES), jnp.float32),
            pltpu.VMEM((group, steps, LANES), jnp.float32),
            pltpu.SemaphoreType.REGULAR((3,)),
            dma((4,)),
            dma((chunks + 1,)),
            dma((chunks + 1,)),
            dma((3,)),
            dma((3,)),
            dma((chunks,)),
            dma((chunks,)),
            dma((chunks,)),
            dma((chunks,)),
            dma((chunks,)),
            dma((chunks,)),
            dma((ring,)),
            dma((ring,)),
            dma((3,)),
            dma((group,)),
        ],
        compiler_params=pltpu.CompilerParams(
            has_side_effects=True, collective_id=0, vmem_limit_bytes=VMEM_LIMIT
        ),
        name="sweep",
    )(
        keep(vol_curve),
        keep(payoff.reshape(rows, LANES)),
        keep(positions.reshape(rows, LANES)),
        keep(offsets),
        keep(tiles),
    )
    groups = curves // SUB
    parts = max(1, rows // (4 * SUB))
    bumped, vega = pl.pallas_call(
        spread_kernel,
        out_shape=(
            jax.ShapeDtypeStruct((groups * rows * SUB, LANES), jnp.float32),
            jax.ShapeDtypeStruct((1, curves), jnp.float32),
        ),
        in_specs=[smem, smem, smem, vmem, vmem],
        out_specs=(pl.BlockSpec(memory_space=pl.ANY), vmem),
        scratch_shapes=[pltpu.VMEM((groups * rows * SUB, LANES), jnp.float32), dma((parts, groups))],
        compiler_params=pltpu.CompilerParams(vmem_limit_bytes=VMEM_LIMIT),
        name="spread",
    )(keep(vol_curve), keep(bucket), keep(bump_size), moved, sums)
    bumped = bumped.reshape(groups, rows, SUB, LANES).transpose(0, 2, 1, 3).reshape(curves, nodes)
    return bumped, vega.reshape(curves)


def solution(mesh):
    shape = dict(mesh.shape)
    in_specs = (
        P(("nx", "ny")),
        P(("nx", "ny")),
        P("bump", None, ("nx", "ny")),
        P(None, ("nx", "ny")),
        P(),
        P("bump"),
        P("bump"),
    )
    out_specs = (P("bump", ("nx", "ny")), P("bump"))
    body = functools.partial(on_device, shape["bump"], shape["nx"], shape["ny"])
    return jax.shard_map(body, mesh=mesh, in_specs=in_specs, out_specs=out_specs, check_vma=False)
```

```python
import functools

import jax
import jax.numpy as jnp
from jax import lax
from jax.experimental import pallas as pl
from jax.experimental.pallas import tpu as pltpu
from jax.sharding import PartitionSpec as P

LANES = 128
SUB = 8
VMEM_LIMIT = 24 * 1024 * 1024
MESH = pl.DeviceIdType.MESH


def sweep_kernel(
    dims,
    curve_ref,
    bucket_ref,
    bump_ref,
    payoff_ref,
    positions_ref,
    offsets_ref,
    tables_ref,
    rows_ref,
    sums_ref,
    vol_ref,
    picks_ref,
    sizes_ref,
    tab,
    pay,
    pos,
    offs,
    coef,
    state,
    mid,
    part,
    tot,
    edge_out,
    edge_in,
    hello,
    loc_sem,
    tab_send,
    tab_recv,
    halo_send,
    halo_recv,
    mid_send,
    mid_recv,
    far_send,
    far_recv,
    near_send,
    near_recv,
    ring_send,
    ring_recv,
    tot_send,
    tot_recv,
):
    n, nx, ny, steps, per, block_len, bounds = dims
    ring_size = nx * ny
    rows = payoff_ref.shape[0]
    blocks = offsets_ref.shape[1]
    comps = tables_ref.shape[0]
    group = n // 2
    half = steps // 2
    share = rows // group
    chunks = len(bounds) - 1
    me = lax.axis_index("bump")
    ring = lax.axis_index("nx") * ny + lax.axis_index("ny")
    side = me // group
    core = lax.rem(me, group)
    upper = side == 1
    lower = side == 0
    first = core == 0

    def at(r, q):
        return {"bump": q, "nx": r // ny, "ny": lax.rem(r, ny)}

    right = lax.rem(ring + 1, ring_size)
    left = lax.rem(ring + ring_size - 1, ring_size)
    sibling = at(ring, side * group + (1 - core))
    across = at(ring, (1 - side) * group + core)
    diagonal = at(ring, (1 - side) * group + (1 - core))
    outer = at(jnp.where(first, right, left), me)

    def start_of(c, a, b):
        return pl.multiple_of(SUB + jnp.where(c == 0, share - b, a), SUB)

    def local(a, b):
        return pl.ds(start_of(core, a, b), b - a)

    def wide_at(c, a, b):
        return pl.ds(pl.multiple_of(start_of(c, a, b) + c * share, SUB), b - a)

    def owned_at(c, a, b):
        return pl.ds(pl.multiple_of(start_of(c, a, b) + c * share - SUB, SUB), b - a)

    def table_at(c, a, b):
        begin = (start_of(c, a, b) + c * share) * per
        return pl.ds(pl.multiple_of(begin, SUB * per), (b - a) * per)

    whole = slice(SUB * per, (SUB + rows) * per)
    loads = [
        pltpu.make_async_copy(tables_ref, tab.at[core, :, whole], loc_sem.at[0]),
        pltpu.make_async_copy(payoff_ref, pay.at[SUB : SUB + rows], loc_sem.at[1]),
        pltpu.make_async_copy(positions_ref, pos, loc_sem.at[2]),
        pltpu.make_async_copy(offsets_ref, offs.at[0], loc_sem.at[3]),
        pltpu.make_async_copy(curve_ref, vol_ref, loc_sem.at[4]),
        pltpu.make_async_copy(bucket_ref, picks_ref, loc_sem.at[5]),
        pltpu.make_async_copy(bump_ref, sizes_ref, loc_sem.at[6]),
    ]

    barrier = pltpu.get_barrier_semaphore()

    def greet(sem, to):
        pl.semaphore_signal(sem, inc=1, device_id=to, device_id_type=MESH)

    keeper = jnp.logical_and(lower, first)
    link = jnp.logical_and(upper, first)
    rest = jnp.logical_not(first)

    @pl.when(link)
    def _():
        greet(barrier, sibling)
        greet(barrier, at(ring, 0))
        greet(barrier, at(left, 0))

    @pl.when(jnp.logical_and(upper, rest))
    def _():
        greet(barrier, at(ring, 0))
        greet(barrier, at(right, 0))

    @pl.when(lower)
    def _():
        greet(barrier, at(ring, group))
        for i in range(1, ring_size):
            greet(barrier, at(lax.rem(ring + i, ring_size), 0))

    @pl.when(keeper)
    def _():
        greet(barrier, sibling)

    for copy in loads:
        copy.start()

    @pl.when(rest)
    def _():
        pl.semaphore_wait(barrier, 1)
        greet(hello.at[0], sibling)

    @pl.when(first)
    def _():
        pl.semaphore_wait(hello.at[0], 1)

    loads[0].wait()

    def remote(src, dst, send, recv, to):
        return pltpu.make_async_remote_copy(
            src_ref=src, dst_ref=dst, send_sem=send, recv_sem=recv, device_id=to, device_id_type=MESH
        )

    def fresh(j):
        lo = -SUB if j == 0 else min(bounds[j] + 2 * SUB, share)
        return lo, min(bounds[j + 1] + 2 * SUB, share)

    table_copies = []
    pieces = [fresh(j) for j in range(chunks)]
    for j, (lo, hi) in enumerate(pieces):
        there = tab.at[core, :, table_at(1 - core, lo, hi)]
        table_copies.append(remote(there, there, tab_send, tab_recv.at[j], sibling))
    edge = pl.multiple_of(jnp.where(first, SUB, rows) * per, SUB * per)
    there = tab.at[core, :, pl.ds(edge, SUB * per)]
    table_copies.append(remote(there, there, tab_send, tab_recv.at[chunks], sibling))
    order = [j for j, (lo, hi) in enumerate(pieces) if lo < hi] + [chunks]
    for j in order:
        table_copies[j].start()

    def arrived(j):
        lo, hi = pieces[j]
        here = tab.at[1 - core, :, table_at(core, lo, hi)]
        return remote(here, here, tab_send, tab_recv.at[j], sibling)

    out_from = pl.multiple_of(jnp.where(first, rows, SUB), SUB)
    out_to = pl.multiple_of(jnp.where(first, 0, rows + SUB), SUB)
    halo_copies = [
        remote(
            pay.at[pl.ds(out_from, SUB)], pay.at[pl.ds(out_to, SUB)],
            halo_send.at[0], halo_recv.at[0], outer,
        ),
        remote(offs.at[0], offs.at[1], halo_send.at[1], halo_recv.at[1], outer),
        remote(edge_out, edge_in, halo_send.at[2], halo_recv.at[2], outer),
    ]

    lines = [(slot, k, (slot * comps + k) * per) for slot in range(group) for k in range(comps)]

    def gather_edge():
        taken = tab.at[1 - core, :, pl.ds(pl.multiple_of(out_from * per, SUB * per), SUB * per)]
        remote(taken, taken, tab_send, tab_recv.at[chunks], sibling).wait_recv()

        @pl.when(first)
        def _():
            for slot, k, line in lines:
                at_row = (SUB + rows - 1) * per
                edge_out[line : line + per, :] = tab[slot, k, at_row : at_row + per, :]

        @pl.when(rest)
        def _():
            for slot, k, line in lines:
                edge_out[line : line + per, :] = tab[slot, k, SUB * per : (SUB + 1) * per, :]

    def place_edge():
        @pl.when(first)
        def _():
            for slot, k, line in lines:
                at_row = (SUB - 1) * per
                tab[slot, k, at_row : at_row + per, :] = edge_in[line : line + per, :]

        @pl.when(rest)
        def _():
            for slot, k, line in lines:
                at_row = (SUB + rows) * per
                tab[slot, k, at_row : at_row + per, :] = edge_in[line : line + per, :]

    loads[3].wait()
    loads[4].wait()

    def prepare(a, b, source):
        count = b - a
        begin = start_of(core, a, b)
        row = lax.broadcasted_iota(jnp.int32, (count, blocks), 0) + (begin - SUB + core * share + rows)
        hit = lax.broadcasted_iota(jnp.int32, (count, blocks), 1) == lax.rem(row, rows) * LANES // block_len
        here = pl.ds(begin, count)
        for t in range(half):
            step = side * half + t
            slot, at_step = t // per, t % per
            line = offs[source, pl.ds(step, 1), :].astype(jnp.float32)
            branch = jnp.sum(jnp.where(hit, line, 0.0), axis=1, keepdims=True)
            branch = jnp.broadcast_to(branch, (count, LANES))
            low = branch < -0.5
            high = branch > 0.5

            def entry(k):
                first_row = (begin + core * share) * per + at_step
                return tab[slot, k, pl.ds(first_row, count, stride=per), :]

            w = vol_ref[step] * vol_ref[step]
            discount = entry(0)
            slope_up = discount * entry(2)
            slope_down = discount * entry(4)
            up = discount * entry(1) + w * slope_up
            down = discount * entry(3) + w * slope_down
            middle = discount - up - down
            slope_mid = -slope_up - slope_down

            def put(k, above, level, below):
                zero = jnp.zeros_like(above)
                coef[t, k, here, :] = jnp.where(high, above, zero)
                coef[t, k + 1, here, :] = jnp.where(high, level, jnp.where(low, zero, above))
                coef[t, k + 2, here, :] = jnp.where(high, below, jnp.where(low, above, level))
                coef[t, k + 3, here, :] = jnp.where(high, zero, jnp.where(low, level, below))
                coef[t, k + 4, here, :] = jnp.where(low, below, zero)

            put(0, up, middle, down)
            put(5, slope_up, slope_mid, slope_down)

    def advance(a, b, top):
        count = b - a
        here = local(a, b)
        lane = lax.broadcasted_iota(jnp.int32, (count, LANES), 1)
        for t in reversed(range(half)):
            s = top + t
            c = [coef[t, k, here, :] for k in range(5)]
            for g in [0] + list(range(s + 2, steps + 1)):
                x = state[g, 0:count, :]
                after = pltpu.roll(x, count - 1, 0)
                before = pltpu.roll(x, 1, 0)
                f1 = pltpu.roll(jnp.where(lane < 1, after, x), LANES - 1, 1)
                f2 = pltpu.roll(jnp.where(lane < 2, after, x), LANES - 2, 1)
                b1 = pltpu.roll(jnp.where(lane >= LANES - 1, before, x), 1, 1)
                b2 = pltpu.roll(jnp.where(lane >= LANES - 2, before, x), 2, 1)
                state[g, 0:count, :] = c[0] * f2 + c[1] * f1 + c[2] * x + c[3] * b1 + c[4] * b2
                if g == 0:
                    e = [coef[t, 5 + k, here, :] for k in range(5)]
                    state[s + 1, 0:count, :] = e[0] * f2 + e[1] * f1 + e[2] * x + e[3] * b1 + e[4] * b2

    passed = [0] + list(range(half + 1, steps + 1))

    def mid_piece(j):
        return (-SUB if j == 0 else bounds[j] + SUB), bounds[j + 1] + SUB

    def mid_copy(j):
        lo, hi = mid_piece(j)
        here = mid.at[:, local(lo, hi)]
        return remote(here, here, mid_send, mid_recv.at[j], across)

    def result_at(c, j):
        return rows_ref.at[:, owned_at(c, bounds[j], bounds[j + 1])]

    def far_copy(j):
        here = result_at(core, j)
        return remote(here, here, far_send, far_recv.at[j], across)

    def near_copy(j):
        here = result_at(core, j)
        return remote(here, here, near_send, near_recv, sibling)

    def all_of(ref, sem):
        pltpu.make_async_copy(ref, ref, sem).wait()

    mine = rows_ref.at[:, owned_at(core, 0, share)]
    others = rows_ref.at[:, owned_at(1 - core, 0, share)]

    @pl.when(upper)
    def _():
        loads[1].wait()
        for j in range(chunks):
            lo, hi = mid_piece(j)
            begin, end = max(lo - SUB, -SUB), min(hi + SUB, share + SUB)
            if pieces[j][0] < pieces[j][1]:
                arrived(j).wait_recv()
                prepare(*pieces[j], 0)
            if j == chunks - 1:
                gather_edge()
                pl.semaphore_wait(hello.at[2], 1)
                for copy in halo_copies:
                    copy.start()
                for copy in halo_copies:
                    copy.wait_recv()
                place_edge()
                prepare(share, share + SUB, 1)
            count = end - begin
            state[0, 0:count, :] = pay[wide_at(core, begin, end), :]
            advance(begin, end, half)
            shift = pl.multiple_of(jnp.where(first, end - hi, lo - begin), SUB)
            for i, g in enumerate(passed):
                mid[i, local(lo, hi), :] = state[g, pl.ds(shift, hi - lo), :]
            if j == 0:

                @pl.when(first)
                def _():
                    pl.semaphore_wait(barrier, 2)
                    greet(hello.at[1], sibling)

                @pl.when(rest)
                def _():
                    pl.semaphore_wait(hello.at[1], 1)

            mid_copy(j).start()
        for copy in halo_copies:
            copy.wait_send()
        for j in range(chunks):
            far_copy(j).wait_recv()
            near_copy(j).start()
        all_of(tot, tot_recv)
        all_of(mid, mid_send)

    @pl.when(lower)
    def _():
        loads[2].wait()
        gather_edge()
        for j in range(chunks):
            if pieces[j][0] < pieces[j][1]:
                arrived(j).wait_recv()
                prepare(*pieces[j], 0)
        for j in range(chunks):
            lo, hi = bounds[j], bounds[j + 1]
            begin, end = lo - SUB, hi + SUB
            if j == 1:

                @pl.when(first)
                def _():
                    pl.semaphore_wait(barrier, 2 * ring_size + 2)
                    greet(hello.at[2], sibling)
                    greet(hello.at[2], across)
                    greet(hello.at[2], diagonal)

            if j == 2:

                @pl.when(rest)
                def _():
                    pl.semaphore_wait(hello.at[2], 1)

            if j == 2:
                for copy in halo_copies[1:]:
                    copy.start()
            if j == chunks - 1:
                for copy in halo_copies[1:]:
                    copy.wait_recv()
                place_edge()
                prepare(share, share + SUB, 1)
            mid_copy(j).wait_recv()
            count = end - begin
            for i, g in enumerate(passed):
                state[g, 0:count, :] = mid[i, local(begin, end), :]
            advance(begin, end, 0)
            here = owned_at(core, lo, hi)
            weights = pos[here, :]
            for g in range(steps + 1):
                center = state[g, SUB : SUB + hi - lo, :]
                rows_ref[g, here, :] = center
                if g:
                    weighted = jnp.sum(weights * center, axis=0, keepdims=True)
                    if j:
                        weighted = weighted + part[ring, g - 1 : g, :]
                    part[ring, g - 1 : g, :] = weighted
            far_copy(j).start()
            near_copy(j).start()
        for i in range(1, ring_size):
            own = part.at[ring]
            remote(own, own, ring_send, ring_recv, at(lax.rem(ring + i, ring_size), me)).start()
        all_of(part.at[1:ring_size], ring_recv)
        tot[core] = jnp.sum(part[...], axis=0)
        total = tot.at[core]
        for to in (sibling, across, diagonal):
            remote(total, total, tot_send, tot_recv, to).start()
        all_of(tot.at[1 - core], tot_recv)
        all_of(part.at[1:ring_size], ring_send)
        all_of(pay.at[0 : 3 * steps], tot_send)
        for copy in halo_copies[1:]:
            copy.wait_send()
        all_of(mine, far_send)

    sums_ref[...] = jnp.sum(tot[...], axis=0)
    all_of(others, near_recv)
    all_of(mine, near_send)
    all_of(tab.at[core, :, 0 : (share + 2 * SUB) * per], tab_send)
    loads[5].wait()
    loads[6].wait()

    @pl.when(upper)
    def _():
        loads[2].wait()

    @pl.when(lower)
    def _():
        loads[1].wait()


def spread_kernel(
    vol_ref, bucket_ref, bump_ref, rows_ref, sums_ref, out_ref, vega_ref, held, small, sem, small_sem
):
    curves = bucket_ref.shape[0]
    groups = curves // SUB
    rows = rows_ref.shape[1]
    parts = sem.shape[0]
    span = rows // parts
    picks = []
    for b in range(curves):
        s = bucket_ref[b]
        slope = 2.0 * vol_ref[s] + bump_ref[b]
        picks.append((s, slope, bump_ref[b] * slope))
    lane = lax.broadcasted_iota(jnp.int32, (1, curves), 1)
    total = jnp.zeros((1, curves), jnp.float32)
    for b in range(curves):
        s, slope, _ = picks[b]
        weighted = jnp.sum(sums_ref[pl.ds(s, 1), :], axis=1, keepdims=True)
        total = jnp.where(lane == b, slope * weighted, total)
    small[...] = total
    copies = [pltpu.make_async_copy(small, vega_ref, small_sem)]
    copies[0].start()
    for i in range(parts):
        here = slice(i * span, (i + 1) * span)
        base = rows_ref[0, here, :]
        for b in range(curves):
            s, _, change = picks[b]
            line = (b // SUB * rows + i * span) * SUB + b % SUB
            held[pl.ds(line, span, stride=SUB), :] = base + change * rows_ref[s + 1, here, :]
        for g in range(groups):
            place = slice((g * rows + i * span) * SUB, (g * rows + (i + 1) * span) * SUB)
            copy = pltpu.make_async_copy(held.at[place], out_ref.at[place], sem.at[i, g])
            copy.start()
            copies.append(copy)
    for copy in copies:
        copy.wait()


def on_device(n, nx, ny, payoff, positions, tables, offsets, vol_curve, bucket, bump_size):
    steps = vol_curve.shape[0]
    per, comps, nodes = tables.shape
    curves = bucket.shape[0]
    rows = nodes // LANES
    block_len = nodes // offsets.shape[1]
    group = n // 2
    share = rows // group
    half = steps // 2
    ring = nx * ny
    bounds = [share * k // (16 * SUB) * SUB for k in (0, 2, 5, 9, 13, 16)]
    chunks = len(bounds) - 1
    widest = max(b - a for a, b in zip(bounds, bounds[1:])) + 3 * SUB
    tiles = tables.transpose(1, 0, 2).reshape(comps, per, rows, LANES).transpose(0, 2, 1, 3)
    tiles = tiles.reshape(comps, rows * per, LANES)
    dma = pltpu.SemaphoreType.DMA
    vmem = pl.BlockSpec(memory_space=pltpu.VMEM)
    smem = pl.BlockSpec(memory_space=pltpu.SMEM)
    hbm = pl.BlockSpec(memory_space=pltpu.HBM)

    def keep(x):
        return pltpu.with_memory_space_constraint(x, pltpu.HBM)

    moved, sums, vol_on, bucket_on, bump_on = pl.pallas_call(
        functools.partial(sweep_kernel, (n, nx, ny, steps, per, block_len, bounds)),
        out_shape=(
            pltpu.VMEM((steps + 1, rows, LANES), jnp.float32),
            pltpu.VMEM((steps, LANES), jnp.float32),
            pltpu.SMEM(vol_curve.shape, vol_curve.dtype),
            pltpu.SMEM(bucket.shape, bucket.dtype),
            pltpu.SMEM(bump_size.shape, bump_size.dtype),
        ),
        in_specs=[hbm] * 7,
        out_specs=(vmem, vmem, smem, smem, smem),
        scratch_shapes=[
            pltpu.VMEM((group, comps, (rows + 2 * SUB) * per, LANES), jnp.float32),
            pltpu.VMEM((rows + 2 * SUB, LANES), jnp.float32),
            pltpu.VMEM((rows, LANES), jnp.float32),
            pltpu.VMEM((2,) + offsets.shape, jnp.int32),
            pltpu.VMEM((half, 10, share + 2 * SUB, LANES), jnp.float32),
            pltpu.VMEM((steps + 1, widest, LANES), jnp.float32),
            pltpu.VMEM((half + 1, share + 2 * SUB, LANES), jnp.float32),
            pltpu.VMEM((ring, steps, LANES), jnp.float32),
            pltpu.VMEM((group, steps, LANES), jnp.float32),
            pltpu.VMEM((group * comps * per, LANES), jnp.float32),
            pltpu.VMEM((group * comps * per, LANES), jnp.float32),
            pltpu.SemaphoreType.REGULAR((3,)),
            dma((7,)),
            dma,
            dma((chunks + 1,)),
            dma((3,)),
            dma((3,)),
            dma,
            dma((chunks,)),
            dma,
            dma((chunks,)),
            dma,
            dma,
            dma,
            dma,
            dma,
            dma,
        ],
        compiler_params=pltpu.CompilerParams(
            has_side_effects=True, collective_id=0, vmem_limit_bytes=VMEM_LIMIT
        ),
        name="sweep",
    )(
        keep(vol_curve),
        keep(bucket),
        keep(bump_size),
        keep(payoff.reshape(rows, LANES)),
        keep(positions.reshape(rows, LANES)),
        keep(offsets),
        keep(tiles),
    )
    groups = curves // SUB
    parts = max(1, rows // (4 * SUB))
    bumped, vega = pl.pallas_call(
        spread_kernel,
        out_shape=(
            jax.ShapeDtypeStruct((groups * rows * SUB, LANES), jnp.float32),
            jax.ShapeDtypeStruct((1, curves), jnp.float32),
        ),
        in_specs=[smem, smem, smem, vmem, vmem],
        out_specs=(pl.BlockSpec(memory_space=pl.ANY), pl.BlockSpec(memory_space=pl.ANY)),
        scratch_shapes=[
            pltpu.VMEM((groups * rows * SUB, LANES), jnp.float32),
            pltpu.VMEM((1, curves), jnp.float32),
            dma((parts, groups)),
            dma,
        ],
        compiler_params=pltpu.CompilerParams(vmem_limit_bytes=VMEM_LIMIT),
        name="spread",
    )(vol_on, bucket_on, bump_on, moved, sums)
    bumped = bumped.reshape(groups, rows, SUB, LANES).transpose(0, 2, 1, 3).reshape(curves, nodes)
    return bumped, vega.reshape(curves)


def solution(mesh):
    shape = dict(mesh.shape)
    in_specs = (
        P(("nx", "ny")),
        P(("nx", "ny")),
        P("bump", None, ("nx", "ny")),
        P(None, ("nx", "ny")),
        P(),
        P("bump"),
        P("bump"),
    )
    out_specs = (P("bump", ("nx", "ny")), P("bump"))
    body = functools.partial(on_device, shape["bump"], shape["nx"], shape["ny"])
    return jax.shard_map(body, mesh=mesh, in_specs=in_specs, out_specs=out_specs, check_vma=False)
```

```python
import functools

import jax
import jax.numpy as jnp
from jax import lax
from jax.experimental import pallas as pl
from jax.experimental.pallas import tpu as pltpu
from jax.sharding import PartitionSpec as P

LANES = 128
SUB = 8
VMEM_LIMIT = 24 * 1024 * 1024
MESH = pl.DeviceIdType.MESH


def sweep_kernel(
    dims,
    curve_ref,
    bucket_ref,
    bump_ref,
    payoff_ref,
    positions_ref,
    offsets_ref,
    tables_ref,
    rows_ref,
    sums_ref,
    vol_ref,
    picks_ref,
    sizes_ref,
    tab,
    pay,
    pos,
    offs,
    coef,
    state,
    mid,
    part,
    tot,
    edge_out,
    edge_in,
    hello,
    loc_sem,
    tab_send,
    tab_recv,
    halo_send,
    halo_recv,
    mid_send,
    mid_recv,
    far_send,
    far_recv,
    near_send,
    near_recv,
    ring_send,
    ring_recv,
    tot_send,
    tot_recv,
):
    n, nx, ny, steps, per, block_len, bounds = dims
    ring_size = nx * ny
    rows = payoff_ref.shape[0]
    blocks = offsets_ref.shape[1]
    comps = tables_ref.shape[0]
    group = n // 2
    half = steps // 2
    share = rows // group
    chunks = len(bounds) - 1
    me = lax.axis_index("bump")
    ring = lax.axis_index("nx") * ny + lax.axis_index("ny")
    side = me // group
    core = lax.rem(me, group)
    upper = side == 1
    lower = side == 0
    first = core == 0

    def at(r, q):
        return {"bump": q, "nx": r // ny, "ny": lax.rem(r, ny)}

    right = lax.rem(ring + 1, ring_size)
    left = lax.rem(ring + ring_size - 1, ring_size)
    sibling = at(ring, side * group + (1 - core))
    across = at(ring, (1 - side) * group + core)
    diagonal = at(ring, (1 - side) * group + (1 - core))
    outer = at(jnp.where(first, right, left), me)

    def start_of(c, a, b):
        return pl.multiple_of(SUB + jnp.where(c == 0, share - b, a), SUB)

    def local(a, b):
        return pl.ds(start_of(core, a, b), b - a)

    def wide_at(c, a, b):
        return pl.ds(pl.multiple_of(start_of(c, a, b) + c * share, SUB), b - a)

    def owned_at(c, a, b):
        return pl.ds(pl.multiple_of(start_of(c, a, b) + c * share - SUB, SUB), b - a)

    def table_at(c, a, b):
        begin = (start_of(c, a, b) + c * share) * per
        return pl.ds(pl.multiple_of(begin, SUB * per), (b - a) * per)

    reach = bounds[1] + 2 * SUB

    def table_load(i, a, b):
        there = tab.at[core, :, (SUB + a) * per : (SUB + b) * per]
        return pltpu.make_async_copy(tables_ref.at[:, a * per : b * per], there, loc_sem.at[i])

    loads = [
        table_load(0, share - reach, share + reach),
        pltpu.make_async_copy(payoff_ref, pay.at[SUB : SUB + rows], loc_sem.at[1]),
        pltpu.make_async_copy(positions_ref, pos, loc_sem.at[2]),
        pltpu.make_async_copy(offsets_ref, offs.at[0], loc_sem.at[3]),
        pltpu.make_async_copy(curve_ref, vol_ref, loc_sem.at[4]),
        pltpu.make_async_copy(bucket_ref, picks_ref, loc_sem.at[5]),
        pltpu.make_async_copy(bump_ref, sizes_ref, loc_sem.at[6]),
        table_load(7, 0, share - reach),
        table_load(8, share + reach, rows),
    ]

    barrier = pltpu.get_barrier_semaphore()

    def greet(sem, to):
        pl.semaphore_signal(sem, inc=1, device_id=to, device_id_type=MESH)

    rest = jnp.logical_not(first)

    for copy in loads[:1] + loads[3:5]:
        copy.start()

    @pl.when(first)
    def _():
        greet(barrier, sibling)
        greet(barrier, at(left, group))

    @pl.when(rest)
    def _():
        greet(barrier, at(right, group))

    @pl.when(upper)
    def _():
        greet(barrier, at(ring, 1))
        loads[1].start()

    for copy in loads[7:]:
        copy.start()

    @pl.when(lower)
    def _():
        for i in range(1, ring_size):
            greet(barrier, at(lax.rem(ring + i, ring_size), 0))
        loads[2].start()

    for copy in loads[5:7]:
        copy.start()

    @pl.when(jnp.logical_and(upper, rest))
    def _():
        pl.semaphore_wait(barrier, 1)
        greet(hello.at[0], sibling)

    @pl.when(jnp.logical_and(lower, rest))
    def _():
        pl.semaphore_wait(barrier, 3)
        greet(hello.at[0], sibling)
        greet(hello.at[1], across)
        greet(hello.at[1], diagonal)

    @pl.when(first)
    def _():
        pl.semaphore_wait(hello.at[0], 1)

    loads[0].wait()

    def remote(src, dst, send, recv, to):
        return pltpu.make_async_remote_copy(
            src_ref=src, dst_ref=dst, send_sem=send, recv_sem=recv, device_id=to, device_id_type=MESH
        )

    def fresh(j):
        lo = -SUB if j == 0 else min(bounds[j] + 2 * SUB, share)
        return lo, min(bounds[j + 1] + 2 * SUB, share)

    table_copies = []
    pieces = [fresh(j) for j in range(chunks)]
    for j, (lo, hi) in enumerate(pieces):
        there = tab.at[core, :, table_at(1 - core, lo, hi)]
        table_copies.append(remote(there, there, tab_send, tab_recv.at[j], sibling))
    edge = pl.multiple_of(jnp.where(first, SUB, rows) * per, SUB * per)
    there = tab.at[core, :, pl.ds(edge, SUB * per)]
    table_copies.append(remote(there, there, tab_send, tab_recv.at[chunks], sibling))
    order = [j for j, (lo, hi) in enumerate(pieces) if lo < hi] + [chunks]
    table_copies[0].start()
    loads[7].wait()
    loads[8].wait()
    for j in order[1:]:
        table_copies[j].start()

    def arrived(j):
        lo, hi = pieces[j]
        here = tab.at[1 - core, :, table_at(core, lo, hi)]
        return remote(here, here, tab_send, tab_recv.at[j], sibling)

    out_from = pl.multiple_of(jnp.where(first, rows, SUB), SUB)
    out_to = pl.multiple_of(jnp.where(first, 0, rows + SUB), SUB)
    halo_copies = [
        remote(
            pay.at[pl.ds(out_from, SUB)], pay.at[pl.ds(out_to, SUB)],
            halo_send.at[0], halo_recv.at[0], outer,
        ),
        remote(offs.at[0], offs.at[1], halo_send.at[1], halo_recv.at[1], outer),
        remote(edge_out, edge_in, halo_send.at[2], halo_recv.at[2], outer),
    ]

    lines = [(slot, k, (slot * comps + k) * per) for slot in range(group) for k in range(comps)]

    def gather_edge():
        taken = tab.at[1 - core, :, pl.ds(pl.multiple_of(out_from * per, SUB * per), SUB * per)]
        remote(taken, taken, tab_send, tab_recv.at[chunks], sibling).wait_recv()

        @pl.when(first)
        def _():
            for slot, k, line in lines:
                at_row = (SUB + rows - 1) * per
                edge_out[line : line + per, :] = tab[slot, k, at_row : at_row + per, :]

        @pl.when(rest)
        def _():
            for slot, k, line in lines:
                edge_out[line : line + per, :] = tab[slot, k, SUB * per : (SUB + 1) * per, :]

    def place_edge():
        @pl.when(first)
        def _():
            for slot, k, line in lines:
                at_row = (SUB - 1) * per
                tab[slot, k, at_row : at_row + per, :] = edge_in[line : line + per, :]

        @pl.when(rest)
        def _():
            for slot, k, line in lines:
                at_row = (SUB + rows) * per
                tab[slot, k, at_row : at_row + per, :] = edge_in[line : line + per, :]

    loads[3].wait()
    loads[4].wait()

    def prepare(a, b, source):
        count = b - a
        begin = start_of(core, a, b)
        row = lax.broadcasted_iota(jnp.int32, (count, blocks), 0) + (begin - SUB + core * share + rows)
        hit = lax.broadcasted_iota(jnp.int32, (count, blocks), 1) == lax.rem(row, rows) * LANES // block_len
        here = pl.ds(begin, count)
        for t in range(half):
            step = side * half + t
            slot, at_step = t // per, t % per
            line = offs[source, pl.ds(step, 1), :].astype(jnp.float32)
            branch = jnp.sum(jnp.where(hit, line, 0.0), axis=1, keepdims=True)
            branch = jnp.broadcast_to(branch, (count, LANES))
            low = branch < -0.5
            high = branch > 0.5

            def entry(k):
                first_row = (begin + core * share) * per + at_step
                return tab[slot, k, pl.ds(first_row, count, stride=per), :]

            w = vol_ref[step] * vol_ref[step]
            discount = entry(0)
            slope_up = discount * entry(2)
            slope_down = discount * entry(4)
            up = discount * entry(1) + w * slope_up
            down = discount * entry(3) + w * slope_down
            middle = discount - up - down
            slope_mid = -slope_up - slope_down

            def put(k, above, level, below):
                zero = jnp.zeros_like(above)
                coef[t, k, here, :] = jnp.where(high, above, zero)
                coef[t, k + 1, here, :] = jnp.where(high, level, jnp.where(low, zero, above))
                coef[t, k + 2, here, :] = jnp.where(high, below, jnp.where(low, above, level))
                coef[t, k + 3, here, :] = jnp.where(high, zero, jnp.where(low, level, below))
                coef[t, k + 4, here, :] = jnp.where(low, below, zero)

            put(0, up, middle, down)
            put(5, slope_up, slope_mid, slope_down)

    def advance(a, b, top):
        count = b - a
        here = local(a, b)
        lane = lax.broadcasted_iota(jnp.int32, (count, LANES), 1)
        for t in reversed(range(half)):
            s = top + t
            c = [coef[t, k, here, :] for k in range(5)]
            for g in [0] + list(range(s + 2, steps + 1)):
                x = state[g, 0:count, :]
                after = pltpu.roll(x, count - 1, 0)
                before = pltpu.roll(x, 1, 0)
                f1 = pltpu.roll(jnp.where(lane < 1, after, x), LANES - 1, 1)
                f2 = pltpu.roll(jnp.where(lane < 2, after, x), LANES - 2, 1)
                b1 = pltpu.roll(jnp.where(lane >= LANES - 1, before, x), 1, 1)
                b2 = pltpu.roll(jnp.where(lane >= LANES - 2, before, x), 2, 1)
                state[g, 0:count, :] = c[0] * f2 + c[1] * f1 + c[2] * x + c[3] * b1 + c[4] * b2
                if g == 0:
                    e = [coef[t, 5 + k, here, :] for k in range(5)]
                    state[s + 1, 0:count, :] = e[0] * f2 + e[1] * f1 + e[2] * x + e[3] * b1 + e[4] * b2

    passed = [0] + list(range(half + 1, steps + 1))

    def mid_piece(j):
        return (-SUB if j == 0 else bounds[j] + SUB), bounds[j + 1] + SUB

    def mid_copy(j):
        lo, hi = mid_piece(j)
        here = mid.at[:, local(lo, hi)]
        return remote(here, here, mid_send, mid_recv.at[j], across)

    def result_at(c, j):
        return rows_ref.at[:, owned_at(c, bounds[j], bounds[j + 1])]

    def far_copy(j):
        here = result_at(core, j)
        return remote(here, here, far_send, far_recv.at[j], across)

    def near_copy(j):
        here = result_at(core, j)
        return remote(here, here, near_send, near_recv, sibling)

    def all_of(ref, sem):
        pltpu.make_async_copy(ref, ref, sem).wait()

    mine = rows_ref.at[:, owned_at(core, 0, share)]
    others = rows_ref.at[:, owned_at(1 - core, 0, share)]

    @pl.when(upper)
    def _():
        loads[1].wait()
        for j in range(chunks):
            lo, hi = mid_piece(j)
            begin, end = max(lo - SUB, -SUB), min(hi + SUB, share + SUB)
            if pieces[j][0] < pieces[j][1]:
                arrived(j).wait_recv()
                prepare(*pieces[j], 0)
            if j == chunks - 1:
                gather_edge()

                @pl.when(first)
                def _():
                    pl.semaphore_wait(barrier, 4)
                    greet(hello.at[2], sibling)
                    greet(hello.at[2], across)
                    greet(hello.at[2], diagonal)

                @pl.when(rest)
                def _():
                    pl.semaphore_wait(hello.at[2], 1)

                for copy in halo_copies:
                    copy.start()
                for copy in halo_copies:
                    copy.wait_recv()
                place_edge()
                prepare(share, share + SUB, 1)
            count = end - begin
            state[0, 0:count, :] = pay[wide_at(core, begin, end), :]
            advance(begin, end, half)
            shift = pl.multiple_of(jnp.where(first, end - hi, lo - begin), SUB)
            for i, g in enumerate(passed):
                mid[i, local(lo, hi), :] = state[g, pl.ds(shift, hi - lo), :]
            if j == 0:
                pl.semaphore_wait(hello.at[1], 1)
            mid_copy(j).start()
        for copy in halo_copies:
            copy.wait_send()
        for j in range(chunks):
            far_copy(j).wait_recv()
            near_copy(j).start()
        all_of(tot, tot_recv)
        all_of(mid, mid_send)

    @pl.when(lower)
    def _():
        loads[2].wait()
        gather_edge()
        for j in range(chunks):
            if pieces[j][0] < pieces[j][1]:
                arrived(j).wait_recv()
                prepare(*pieces[j], 0)
        for j in range(chunks):
            lo, hi = bounds[j], bounds[j + 1]
            begin, end = lo - SUB, hi + SUB
            if j == 2:
                pl.semaphore_wait(hello.at[2], 1)
                for copy in halo_copies[1:]:
                    copy.start()
            if j == chunks - 1:
                for copy in halo_copies[1:]:
                    copy.wait_recv()
                place_edge()
                prepare(share, share + SUB, 1)
            mid_copy(j).wait_recv()
            count = end - begin
            for i, g in enumerate(passed):
                state[g, 0:count, :] = mid[i, local(begin, end), :]
            advance(begin, end, 0)
            here = owned_at(core, lo, hi)
            weights = pos[here, :]
            for g in range(steps + 1):
                center = state[g, SUB : SUB + hi - lo, :]
                rows_ref[g, here, :] = center
                if g:
                    weighted = jnp.sum(weights * center, axis=0, keepdims=True)
                    if j:
                        weighted = weighted + part[ring, g - 1 : g, :]
                    part[ring, g - 1 : g, :] = weighted
            far_copy(j).start()
            near_copy(j).start()

        @pl.when(first)
        def _():
            pl.semaphore_wait(barrier, 2 * ring_size - 2)
            greet(hello.at[3], sibling)

        @pl.when(rest)
        def _():
            pl.semaphore_wait(hello.at[3], 1)

        for i in range(1, ring_size):
            own = part.at[ring]
            remote(own, own, ring_send, ring_recv, at(lax.rem(ring + i, ring_size), me)).start()
        all_of(part.at[1:ring_size], ring_recv)
        tot[core] = jnp.sum(part[...], axis=0)
        total = tot.at[core]
        for to in (sibling, across, diagonal):
            remote(total, total, tot_send, tot_recv, to).start()
        all_of(tot.at[1 - core], tot_recv)
        all_of(part.at[1:ring_size], ring_send)
        all_of(pay.at[0 : 3 * steps], tot_send)
        for copy in halo_copies[1:]:
            copy.wait_send()
        all_of(mine, far_send)

    sums_ref[...] = jnp.sum(tot[...], axis=0)
    all_of(others, near_recv)
    all_of(mine, near_send)
    all_of(tab.at[core, :, 0 : (share + 2 * SUB) * per], tab_send)
    loads[5].wait()
    loads[6].wait()

def spread_kernel(
    vol_ref, bucket_ref, bump_ref, rows_ref, sums_ref, out_ref, vega_ref, held, small, sem, small_sem
):
    curves = bucket_ref.shape[0]
    groups = curves // SUB
    rows = rows_ref.shape[1]
    parts = sem.shape[0]
    span = rows // parts
    picks = []
    for b in range(curves):
        s = bucket_ref[b]
        slope = 2.0 * vol_ref[s] + bump_ref[b]
        picks.append((s, slope, bump_ref[b] * slope))
    lane = lax.broadcasted_iota(jnp.int32, (1, curves), 1)
    total = jnp.zeros((1, curves), jnp.float32)
    for b in range(curves):
        s, slope, _ = picks[b]
        weighted = jnp.sum(sums_ref[pl.ds(s, 1), :], axis=1, keepdims=True)
        total = jnp.where(lane == b, slope * weighted, total)
    small[...] = total
    copies = [pltpu.make_async_copy(small, vega_ref, small_sem)]
    copies[0].start()
    for i in range(parts):
        here = slice(i * span, (i + 1) * span)
        base = rows_ref[0, here, :]
        for b in range(curves):
            s, _, change = picks[b]
            line = (b // SUB * rows + i * span) * SUB + b % SUB
            held[pl.ds(line, span, stride=SUB), :] = base + change * rows_ref[s + 1, here, :]
        for g in range(groups):
            place = slice((g * rows + i * span) * SUB, (g * rows + (i + 1) * span) * SUB)
            copy = pltpu.make_async_copy(held.at[place], out_ref.at[place], sem.at[i, g])
            copy.start()
            copies.append(copy)
    for copy in copies:
        copy.wait()


def on_device(n, nx, ny, payoff, positions, tables, offsets, vol_curve, bucket, bump_size):
    steps = vol_curve.shape[0]
    per, comps, nodes = tables.shape
    curves = bucket.shape[0]
    rows = nodes // LANES
    block_len = nodes // offsets.shape[1]
    group = n // 2
    share = rows // group
    half = steps // 2
    ring = nx * ny
    bounds = [share * k // (16 * SUB) * SUB for k in (0, 1, 3, 6, 10, 13, 16)]
    chunks = len(bounds) - 1
    widest = max(b - a for a, b in zip(bounds, bounds[1:])) + 3 * SUB
    tiles = tables.transpose(1, 0, 2).reshape(comps, per, rows, LANES).transpose(0, 2, 1, 3)
    tiles = tiles.reshape(comps, rows * per, LANES)
    dma = pltpu.SemaphoreType.DMA
    vmem = pl.BlockSpec(memory_space=pltpu.VMEM)
    smem = pl.BlockSpec(memory_space=pltpu.SMEM)
    hbm = pl.BlockSpec(memory_space=pltpu.HBM)

    def keep(x):
        return pltpu.with_memory_space_constraint(x, pltpu.HBM)

    moved, sums, vol_on, bucket_on, bump_on = pl.pallas_call(
        functools.partial(sweep_kernel, (n, nx, ny, steps, per, block_len, bounds)),
        out_shape=(
            pltpu.VMEM((steps + 1, rows, LANES), jnp.float32),
            pltpu.VMEM((steps, LANES), jnp.float32),
            pltpu.SMEM(vol_curve.shape, vol_curve.dtype),
            pltpu.SMEM(bucket.shape, bucket.dtype),
            pltpu.SMEM(bump_size.shape, bump_size.dtype),
        ),
        in_specs=[hbm] * 7,
        out_specs=(vmem, vmem, smem, smem, smem),
        scratch_shapes=[
            pltpu.VMEM((group, comps, (rows + 2 * SUB) * per, LANES), jnp.float32),
            pltpu.VMEM((rows + 2 * SUB, LANES), jnp.float32),
            pltpu.VMEM((rows, LANES), jnp.float32),
            pltpu.VMEM((2,) + offsets.shape, jnp.int32),
            pltpu.VMEM((half, 10, share + 2 * SUB, LANES), jnp.float32),
            pltpu.VMEM((steps + 1, widest, LANES), jnp.float32),
            pltpu.VMEM((half + 1, share + 2 * SUB, LANES), jnp.float32),
            pltpu.VMEM((ring, steps, LANES), jnp.float32),
            pltpu.VMEM((group, steps, LANES), jnp.float32),
            pltpu.VMEM((group * comps * per, LANES), jnp.float32),
            pltpu.VMEM((group * comps * per, LANES), jnp.float32),
            pltpu.SemaphoreType.REGULAR((4,)),
            dma((9,)),
            dma,
            dma((chunks + 1,)),
            dma((3,)),
            dma((3,)),
            dma,
            dma((chunks,)),
            dma,
            dma((chunks,)),
            dma,
            dma,
            dma,
            dma,
            dma,
            dma,
        ],
        compiler_params=pltpu.CompilerParams(
            has_side_effects=True, collective_id=0, vmem_limit_bytes=VMEM_LIMIT
        ),
        name="sweep",
    )(
        keep(vol_curve),
        keep(bucket),
        keep(bump_size),
        keep(payoff.reshape(rows, LANES)),
        keep(positions.reshape(rows, LANES)),
        keep(offsets),
        keep(tiles),
    )
    groups = curves // SUB
    parts = max(1, rows // (4 * SUB))
    bumped, vega = pl.pallas_call(
        spread_kernel,
        out_shape=(
            jax.ShapeDtypeStruct((groups * rows * SUB, LANES), jnp.float32),
            jax.ShapeDtypeStruct((1, curves), jnp.float32),
        ),
        in_specs=[smem, smem, smem, vmem, vmem],
        out_specs=(pl.BlockSpec(memory_space=pl.ANY), pl.BlockSpec(memory_space=pl.ANY)),
        scratch_shapes=[
            pltpu.VMEM((groups * rows * SUB, LANES), jnp.float32),
            pltpu.VMEM((1, curves), jnp.float32),
            dma((parts, groups)),
            dma,
        ],
        compiler_params=pltpu.CompilerParams(vmem_limit_bytes=VMEM_LIMIT),
        name="spread",
    )(vol_on, bucket_on, bump_on, moved, sums)
    bumped = bumped.reshape(groups, rows, SUB, LANES).transpose(0, 2, 1, 3).reshape(curves, nodes)
    return bumped, vega.reshape(curves)


def solution(mesh):
    shape = dict(mesh.shape)
    in_specs = (
        P(("nx", "ny")),
        P(("nx", "ny")),
        P("bump", None, ("nx", "ny")),
        P(None, ("nx", "ny")),
        P(),
        P("bump"),
        P("bump"),
    )
    out_specs = (P("bump", ("nx", "ny")), P("bump"))
    body = functools.partial(on_device, shape["bump"], shape["nx"], shape["ny"])
    return jax.shard_map(body, mesh=mesh, in_specs=in_specs, out_specs=out_specs, check_vma=False)
```

```python
import functools

import jax
import jax.numpy as jnp
from jax import lax
from jax.experimental import pallas as pl
from jax.experimental.pallas import tpu as pltpu
from jax.sharding import PartitionSpec as P

LANES = 128
SUB = 8
VMEM_LIMIT = 24 * 1024 * 1024
MESH = pl.DeviceIdType.MESH


def sweep_kernel(
    dims,
    curve_ref,
    bucket_ref,
    bump_ref,
    payoff_ref,
    positions_ref,
    offsets_ref,
    tables_ref,
    lines_ref,
    rows_ref,
    sums_ref,
    vol_ref,
    picks_ref,
    sizes_ref,
    tab,
    pay,
    pos,
    offs,
    coef,
    state,
    mid,
    part,
    gathered,
    strip_sum,
    total,
    edge_out,
    edge_in,
    lent,
    hello,
    loc_sem,
    lent_send,
    lent_recv,
    tab_send,
    tab_recv,
    halo_send,
    halo_recv,
    mid_send,
    mid_recv,
    far_send,
    far_recv,
    near_send,
    near_recv,
    ring_send,
    ring_recv,
    strip_send,
    strip_recv,
    tot_send,
    tot_recv,
):
    n, nx, ny, steps, per, block_len, bounds, strip = dims
    ring_size = nx * ny
    rows = payoff_ref.shape[0]
    blocks = offsets_ref.shape[1]
    comps = tables_ref.shape[0]
    group = n // 2
    half = steps // 2
    share = rows // group
    chunks = len(bounds) - 1
    me = lax.axis_index("bump")
    ring = lax.axis_index("nx") * ny + lax.axis_index("ny")
    side = me // group
    core = lax.rem(me, group)
    upper = side == 1
    lower = side == 0
    first = core == 0

    def at(r, q):
        return {"bump": q, "nx": r // ny, "ny": lax.rem(r, ny)}

    right = lax.rem(ring + 1, ring_size)
    left = lax.rem(ring + ring_size - 1, ring_size)
    sibling = at(ring, side * group + (1 - core))
    across = at(ring, (1 - side) * group + core)
    diagonal = at(ring, (1 - side) * group + (1 - core))
    outer = at(jnp.where(first, right, left), me)

    def start_of(c, a, b):
        return pl.multiple_of(SUB + jnp.where(c == 0, share - b, a), SUB)

    def local(a, b):
        return pl.ds(start_of(core, a, b), b - a)

    def wide_at(c, a, b):
        return pl.ds(pl.multiple_of(start_of(c, a, b) + c * share, SUB), b - a)

    def owned_at(c, a, b):
        return pl.ds(pl.multiple_of(start_of(c, a, b) + c * share - SUB, SUB), b - a)

    def table_at(c, a, b):
        begin = (start_of(c, a, b) + c * share) * per
        return pl.ds(pl.multiple_of(begin, SUB * per), (b - a) * per)

    reach = bounds[1] + 2 * SUB

    def table_load(i, a, b):
        there = tab.at[core, :, (SUB + a) * per : (SUB + b) * per]
        return pltpu.make_async_copy(tables_ref.at[:, a * per : b * per], there, loc_sem.at[i])

    loads = [
        table_load(0, share - reach, share + reach),
        pltpu.make_async_copy(payoff_ref, pay.at[SUB : SUB + rows], loc_sem.at[1]),
        pltpu.make_async_copy(positions_ref, pos, loc_sem.at[2]),
        pltpu.make_async_copy(offsets_ref, offs.at[0], loc_sem.at[3]),
        pltpu.make_async_copy(curve_ref, vol_ref, loc_sem.at[4]),
        pltpu.make_async_copy(bucket_ref, picks_ref, loc_sem.at[5]),
        pltpu.make_async_copy(bump_ref, sizes_ref, loc_sem.at[6]),
        table_load(7, 0, share - reach),
        table_load(8, share + reach, rows),
    ]

    barrier = pltpu.get_barrier_semaphore()

    def greet(sem, to):
        pl.semaphore_signal(sem, inc=1, device_id=to, device_id_type=MESH)

    rest = jnp.logical_not(first)

    for copy in loads[:1] + loads[3:5]:
        copy.start()

    @pl.when(first)
    def _():
        greet(barrier, sibling)
        greet(barrier, at(left, group))

    @pl.when(rest)
    def _():
        greet(barrier, at(right, group))

    @pl.when(upper)
    def _():
        greet(barrier, at(ring, 1))
        loads[1].start()
        loads[2].start()

    for copy in loads[7:]:
        copy.start()

    @pl.when(lower)
    def _():
        for i in range(1, ring_size):
            greet(barrier, at(lax.rem(ring + i, ring_size), 0))
        loads[2].start()

    for copy in loads[5:7]:
        copy.start()

    @pl.when(jnp.logical_and(upper, rest))
    def _():
        pl.semaphore_wait(barrier, 1)
        greet(hello.at[0], sibling)

    @pl.when(jnp.logical_and(lower, rest))
    def _():
        pl.semaphore_wait(barrier, 3)
        greet(hello.at[0], sibling)
        greet(hello.at[1], across)
        greet(hello.at[1], diagonal)

    @pl.when(first)
    def _():
        pl.semaphore_wait(hello.at[0], 1)

    loads[0].wait()

    def remote(src, dst, send, recv, to):
        return pltpu.make_async_remote_copy(
            src_ref=src, dst_ref=dst, send_sem=send, recv_sem=recv, device_id=to, device_id_type=MESH
        )

    def fresh(j):
        lo = -SUB if j == 0 else min(bounds[j] + 2 * SUB, share)
        return lo, min(bounds[j + 1] + 2 * SUB, share)

    from_row, to_row = bounds[strip], bounds[strip + 1]
    lent_rows = to_row - from_row + 2

    def lend(c, to):
        begin = c * share + jnp.where(c == 0, share - to_row, from_row) - 1
        source = lines_ref.at[:, pl.ds(begin, lent_rows)]
        there = lent.at[core, :, SUB - 1 : SUB - 1 + lent_rows]
        return remote(source, there, lent_send, lent_recv, to)

    @pl.when(lower)
    def _():
        lend(core, across).start()
        lend(1 - core, diagonal).start()

    def all_of(ref, sem):
        pltpu.make_async_copy(ref, ref, sem).wait()

    table_copies = []
    pieces = [fresh(j) for j in range(chunks)]
    for j, (lo, hi) in enumerate(pieces):
        there = tab.at[core, :, table_at(1 - core, lo, hi)]
        table_copies.append(remote(there, there, tab_send, tab_recv.at[j], sibling))
    edge = pl.multiple_of(jnp.where(first, SUB, rows) * per, SUB * per)
    there = tab.at[core, :, pl.ds(edge, SUB * per)]
    table_copies.append(remote(there, there, tab_send, tab_recv.at[chunks], sibling))
    order = [j for j, (lo, hi) in enumerate(pieces) if lo < hi] + [chunks]
    table_copies[0].start()
    loads[7].wait()
    loads[8].wait()
    for j in order[1:]:
        table_copies[j].start()

    def arrived(j):
        lo, hi = pieces[j]
        here = tab.at[1 - core, :, table_at(core, lo, hi)]
        return remote(here, here, tab_send, tab_recv.at[j], sibling)

    out_from = pl.multiple_of(jnp.where(first, rows, SUB), SUB)
    out_to = pl.multiple_of(jnp.where(first, 0, rows + SUB), SUB)
    halo_copies = [
        remote(
            pay.at[pl.ds(out_from, SUB)], pay.at[pl.ds(out_to, SUB)],
            halo_send.at[0], halo_recv.at[0], outer,
        ),
        remote(offs.at[0], offs.at[1], halo_send.at[1], halo_recv.at[1], outer),
        remote(edge_out, edge_in, halo_send.at[2], halo_recv.at[2], outer),
    ]

    lines = [(slot, k, (slot * comps + k) * per) for slot in range(group) for k in range(comps)]

    def gather_edge():
        taken = tab.at[1 - core, :, pl.ds(pl.multiple_of(out_from * per, SUB * per), SUB * per)]
        remote(taken, taken, tab_send, tab_recv.at[chunks], sibling).wait_recv()

        @pl.when(first)
        def _():
            for slot, k, line in lines:
                at_row = (SUB + rows - 1) * per
                edge_out[line : line + per, :] = tab[slot, k, at_row : at_row + per, :]

        @pl.when(rest)
        def _():
            for slot, k, line in lines:
                edge_out[line : line + per, :] = tab[slot, k, SUB * per : (SUB + 1) * per, :]

    def place_edge():
        @pl.when(first)
        def _():
            for slot, k, line in lines:
                at_row = (SUB - 1) * per
                tab[slot, k, at_row : at_row + per, :] = edge_in[line : line + per, :]

        @pl.when(rest)
        def _():
            for slot, k, line in lines:
                at_row = (SUB + rows) * per
                tab[slot, k, at_row : at_row + per, :] = edge_in[line : line + per, :]

    loads[3].wait()
    loads[4].wait()

    def prepare(a, b, source, borrowed=False):
        count = b - a
        begin = start_of(core, a, b)
        row = lax.broadcasted_iota(jnp.int32, (count, blocks), 0) + (begin - SUB + core * share + rows)
        hit = lax.broadcasted_iota(jnp.int32, (count, blocks), 1) == lax.rem(row, rows) * LANES // block_len
        here = pl.ds(begin, count)
        for t in range(half):
            step = t if borrowed else side * half + t
            slot, at_step = t // per, t % per
            line = offs[source, pl.ds(step, 1), :].astype(jnp.float32)
            branch = jnp.sum(jnp.where(hit, line, 0.0), axis=1, keepdims=True)
            branch = jnp.broadcast_to(branch, (count, LANES))
            low = branch < -0.5
            high = branch > 0.5

            def entry(k):
                if borrowed:
                    return lent[slot, k, 0:count, at_step, :]
                first_row = (begin + core * share) * per + at_step
                return tab[slot, k, pl.ds(first_row, count, stride=per), :]

            w = vol_ref[step] * vol_ref[step]
            discount = entry(0)
            slope_up = discount * entry(2)
            slope_down = discount * entry(4)
            up = discount * entry(1) + w * slope_up
            down = discount * entry(3) + w * slope_down
            middle = discount - up - down
            slope_mid = -slope_up - slope_down

            def put(k, above, level, below):
                zero = jnp.zeros_like(above)
                coef[t, k, here, :] = jnp.where(high, above, zero)
                coef[t, k + 1, here, :] = jnp.where(high, level, jnp.where(low, zero, above))
                coef[t, k + 2, here, :] = jnp.where(high, below, jnp.where(low, above, level))
                coef[t, k + 3, here, :] = jnp.where(high, zero, jnp.where(low, level, below))
                coef[t, k + 4, here, :] = jnp.where(low, below, zero)

            put(0, up, middle, down)
            put(5, slope_up, slope_mid, slope_down)

    def advance(a, b, top):
        count = b - a
        here = local(a, b)
        lane = lax.broadcasted_iota(jnp.int32, (count, LANES), 1)
        for t in reversed(range(half)):
            s = top + t
            c = [coef[t, k, here, :] for k in range(5)]
            for g in [0] + list(range(s + 2, steps + 1)):
                x = state[g, 0:count, :]
                after = pltpu.roll(x, count - 1, 0)
                before = pltpu.roll(x, 1, 0)
                f1 = pltpu.roll(jnp.where(lane < 1, after, x), LANES - 1, 1)
                f2 = pltpu.roll(jnp.where(lane < 2, after, x), LANES - 2, 1)
                b1 = pltpu.roll(jnp.where(lane >= LANES - 1, before, x), 1, 1)
                b2 = pltpu.roll(jnp.where(lane >= LANES - 2, before, x), 2, 1)
                state[g, 0:count, :] = c[0] * f2 + c[1] * f1 + c[2] * x + c[3] * b1 + c[4] * b2
                if g == 0:
                    e = [coef[t, 5 + k, here, :] for k in range(5)]
                    state[s + 1, 0:count, :] = e[0] * f2 + e[1] * f1 + e[2] * x + e[3] * b1 + e[4] * b2

    passed = [0] + list(range(half + 1, steps + 1))

    def mid_piece(j):
        return (-SUB if j == 0 else bounds[j] + SUB), bounds[j + 1] + SUB

    def mid_copy(j, c):
        lo = -1 if j == 0 else bounds[j] + 1
        hi = bounds[j + 1] + 1
        begin = SUB + (share - hi if c == 0 else lo)
        here = mid.at[:, begin : begin + hi - lo]
        return remote(here, here, mid_send, mid_recv.at[j], across)

    def each_core(act):
        @pl.when(first)
        def _():
            act(0)

        @pl.when(rest)
        def _():
            act(1)

    def result_at(c, j):
        return rows_ref.at[:, owned_at(c, bounds[j], bounds[j + 1])]

    def far_copy(j):
        here = result_at(core, j)
        return remote(here, here, far_send, far_recv.at[j], across)

    def near_copy(j):
        here = result_at(core, j)
        return remote(here, here, near_send, near_recv, sibling)

    def weigh(g, here, fresh):
        weighted = jnp.sum(pos[here, :] * rows_ref[g, here, :], axis=0, keepdims=True)
        part[g - 1 : g, :] = weighted if fresh else part[g - 1 : g, :] + weighted

    def packed():
        each = jnp.broadcast_to(jnp.sum(part[...], axis=1, keepdims=True), (steps, LANES))
        place = lax.broadcasted_iota(jnp.int32, (steps, LANES), 0)
        lane = lax.broadcasted_iota(jnp.int32, (steps, LANES), 1)
        return jnp.sum(jnp.where(place == lane, each, 0.0), axis=0, keepdims=True)

    strip_copy = remote(strip_sum.at[0], strip_sum.at[1], strip_send, strip_recv, across)
    def total_copy(to):
        return remote(total.at[0], total.at[1], tot_send, tot_recv, to)


    mine = rows_ref.at[:, owned_at(core, 0, share)]
    others = rows_ref.at[:, owned_at(1 - core, 0, share)]

    wrapped = lax.axis_index("ny") == 0

    def send_halos():
        gather_edge()

        @pl.when(first)
        def _():
            pl.semaphore_wait(barrier, 4)
            greet(hello.at[2], sibling)
            greet(hello.at[2], across)
            greet(hello.at[2], diagonal)

        @pl.when(rest)
        def _():
            pl.semaphore_wait(hello.at[2], 1)

        for copy in halo_copies:
            copy.start()

    @pl.when(upper)
    def _():
        loads[1].wait()
        for j in range(chunks):
            lo, hi = mid_piece(j)
            begin, end = max(lo - SUB, -SUB), min(hi + SUB, share + SUB)
            if pieces[j][0] < pieces[j][1]:
                arrived(j).wait_recv()
                prepare(*pieces[j], 0)
            if j == chunks - 1:
                pl.when(wrapped)(send_halos)
                for copy in halo_copies:
                    copy.wait_recv()
                place_edge()
                prepare(share, share + SUB, 1)
            count = end - begin
            state[0, 0:count, :] = pay[wide_at(core, begin, end), :]
            advance(begin, end, half)
            shift = pl.multiple_of(jnp.where(first, end - hi, lo - begin), SUB)
            for i, g in enumerate(passed):
                mid[i, local(lo, hi), :] = state[g, pl.ds(shift, hi - lo), :]
            if j == 0:
                pl.semaphore_wait(hello.at[1], 1)
            each_core(lambda c: mid_copy(j, c).start())
            if j == 1:
                pl.when(jnp.logical_not(wrapped))(send_halos)
        loads[2].wait()
        all_of(lent.at[:, :, SUB - 1 : SUB - 1 + lent_rows], lent_recv)
        begin, end = from_row - SUB, to_row + SUB
        prepare(begin, end, 0, True)
        for i, g in enumerate(passed):
            state[g, 0 : end - begin, :] = mid[i, local(begin, end), :]
        advance(begin, end, 0)
        for g in range(steps + 1):
            rows_ref[g, owned_at(core, from_row, to_row), :] = state[g, SUB : end - begin - SUB, :]
            if g:
                weigh(g, owned_at(core, from_row, to_row), True)
        strip_sum[0] = packed()
        strip_copy.start()
        far_copy(strip).start()
        near_copy(strip).start()
        for copy in halo_copies:
            copy.wait_send()
        for j in range(chunks):
            if j != strip:
                far_copy(j).wait_recv()
                near_copy(j).start()
        total_copy(across).wait_recv()
        sums_ref[...] = total[1]
        strip_copy.wait_send()
        all_of(mid.at[:, 0 : share + 2], mid_send)
        far_copy(strip).wait_send()

    @pl.when(lower)
    def _():
        loads[2].wait()
        gather_edge()
        for j in range(chunks):
            if pieces[j][0] < pieces[j][1]:
                arrived(j).wait_recv()
                prepare(*pieces[j], 0)
        for j in range(chunks):
            lo, hi = bounds[j], bounds[j + 1]
            begin, end = lo - SUB, hi + SUB
            if j == 0:
                pl.semaphore_wait(hello.at[2], 1)
                for copy in halo_copies[1:]:
                    copy.start()
            if j == strip:
                mid_copy(j, 0).wait_recv()

                @pl.when(first)
                def _():
                    pl.semaphore_wait(barrier, 2 * ring_size - 2)
                    greet(hello.at[3], sibling)

                continue
            if j == chunks - 1:
                for copy in halo_copies[1:]:
                    copy.wait_recv()
                place_edge()
                prepare(share, share + SUB, 1)
            mid_copy(j, 0).wait_recv()
            count = end - begin

            def take(c):
                skip = SUB - 1
                start = share - hi if c == 0 else lo
                a, b = (skip, count) if c == 0 else (0, count - skip)
                for i, g in enumerate(passed):
                    state[g, a:b, :] = mid[i, start + a : start + b, :]

            each_core(take)
            advance(begin, end, 0)
            here = owned_at(core, lo, hi)
            for g in range(steps + 1):
                rows_ref[g, here, :] = state[g, SUB : SUB + hi - lo, :]
            far_copy(j).start()
            near_copy(j).start()
            for g in range(1, steps + 1):
                weigh(g, here, j == 0)

        strip_copy.wait_recv()
        own = core * ring_size + ring
        gathered[own] = packed() + strip_sum[1]

        @pl.when(rest)
        def _():
            pl.semaphore_wait(hello.at[3], 1)

        for i in range(1, ring_size):
            for c in range(group):
                to = at(lax.rem(ring + i, ring_size), c)
                remote(gathered.at[own], gathered.at[own], ring_send, ring_recv, to).start()
        remote(gathered.at[own], gathered.at[own], ring_send, ring_recv, sibling).start()
        far_copy(strip).wait_recv()
        near_copy(strip).start()
        all_of(gathered.at[1 : group * ring_size], ring_recv)
        total[0] = jnp.sum(gathered[...], axis=0)

        @pl.when(rest)
        def _():
            total_copy(across).start()
            total_copy(diagonal).start()

        sums_ref[...] = total[0]
        all_of(gathered.at[1 : group * ring_size], ring_send)

        @pl.when(rest)
        def _():
            all_of(gathered.at[0:2], tot_send)

        for copy in halo_copies[1:]:
            copy.wait_send()
        all_of(rows_ref.at[:, owned_at(core, 0, share - (to_row - from_row))], far_send)
        all_of(lent.at[:, :, SUB - 1 : SUB - 1 + lent_rows], lent_send)

    all_of(others, near_recv)
    all_of(mine, near_send)
    all_of(tab.at[core, :, 0 : (share + 2 * SUB) * per], tab_send)
    loads[5].wait()
    loads[6].wait()

def spread_kernel(
    vol_ref, bucket_ref, bump_ref, rows_ref, sums_ref, out_ref, vega_ref, held, small, sem, small_sem
):
    curves = bucket_ref.shape[0]
    groups = curves // SUB
    rows = rows_ref.shape[1]
    parts = sem.shape[0]
    span = rows // parts
    picks = []
    for b in range(curves):
        s = bucket_ref[b]
        slope = 2.0 * vol_ref[s] + bump_ref[b]
        picks.append((s, slope, bump_ref[b] * slope))
    lane = lax.broadcasted_iota(jnp.int32, (1, curves), 1)
    spot = lax.broadcasted_iota(jnp.int32, (1, LANES), 1)
    total = jnp.zeros((1, curves), jnp.float32)
    for b in range(curves):
        s, slope, _ = picks[b]
        weighted = jnp.sum(jnp.where(spot == s, sums_ref[...], 0.0), axis=1, keepdims=True)
        total = jnp.where(lane == b, slope * weighted, total)
    small[...] = total
    copies = [pltpu.make_async_copy(small, vega_ref, small_sem)]
    copies[0].start()
    for i in range(parts):
        here = slice(i * span, (i + 1) * span)
        base = rows_ref[0, here, :]
        for b in range(curves):
            s, _, change = picks[b]
            line = (b // SUB * rows + i * span) * SUB + b % SUB
            held[pl.ds(line, span, stride=SUB), :] = base + change * rows_ref[s + 1, here, :]
        for g in range(groups):
            place = slice((g * rows + i * span) * SUB, (g * rows + (i + 1) * span) * SUB)
            copy = pltpu.make_async_copy(held.at[place], out_ref.at[place], sem.at[i, g])
            copy.start()
            copies.append(copy)
    for copy in copies:
        copy.wait()


def on_device(n, nx, ny, payoff, positions, tables, offsets, vol_curve, bucket, bump_size):
    steps = vol_curve.shape[0]
    per, comps, nodes = tables.shape
    curves = bucket.shape[0]
    rows = nodes // LANES
    block_len = nodes // offsets.shape[1]
    group = n // 2
    share = rows // group
    half = steps // 2
    ring = nx * ny
    bounds = [share * k // (16 * SUB) * SUB for k in (0, 1, 3, 6, 10, 12, 16)]
    strip = 4
    chunks = len(bounds) - 1
    widest = max(b - a for a, b in zip(bounds, bounds[1:])) + 3 * SUB
    lines = tables.transpose(1, 0, 2).reshape(comps, per, rows, LANES).transpose(0, 2, 1, 3)
    tiles = lines.reshape(comps, rows * per, LANES)
    dma = pltpu.SemaphoreType.DMA
    vmem = pl.BlockSpec(memory_space=pltpu.VMEM)
    smem = pl.BlockSpec(memory_space=pltpu.SMEM)
    hbm = pl.BlockSpec(memory_space=pltpu.HBM)

    def keep(x):
        return pltpu.with_memory_space_constraint(x, pltpu.HBM)

    moved, sums, vol_on, bucket_on, bump_on = pl.pallas_call(
        functools.partial(sweep_kernel, (n, nx, ny, steps, per, block_len, bounds, strip)),
        out_shape=(
            pltpu.VMEM((steps + 1, rows, LANES), jnp.float32),
            pltpu.VMEM((1, LANES), jnp.float32),
            pltpu.SMEM(vol_curve.shape, vol_curve.dtype),
            pltpu.SMEM(bucket.shape, bucket.dtype),
            pltpu.SMEM(bump_size.shape, bump_size.dtype),
        ),
        in_specs=[hbm] * 8,
        out_specs=(vmem, vmem, smem, smem, smem),
        scratch_shapes=[
            pltpu.VMEM((group, comps, (rows + 2 * SUB) * per, LANES), jnp.float32),
            pltpu.VMEM((rows + 2 * SUB, LANES), jnp.float32),
            pltpu.VMEM((rows, LANES), jnp.float32),
            pltpu.VMEM((2,) + offsets.shape, jnp.int32),
            pltpu.VMEM((half, 10, share + 2 * SUB, LANES), jnp.float32),
            pltpu.VMEM((steps + 1, widest, LANES), jnp.float32),
            pltpu.VMEM((half + 1, share + 2 * SUB, LANES), jnp.float32),
            pltpu.VMEM((steps, LANES), jnp.float32),
            pltpu.VMEM((group * ring, 1, LANES), jnp.float32),
            pltpu.VMEM((2, 1, LANES), jnp.float32),
            pltpu.VMEM((2, 1, LANES), jnp.float32),
            pltpu.VMEM((group * comps * per, LANES), jnp.float32),
            pltpu.VMEM((group * comps * per, LANES), jnp.float32),
            pltpu.VMEM(
                (group, comps, bounds[strip + 1] - bounds[strip] + 2 * SUB, per, LANES), jnp.float32
            ),
            pltpu.SemaphoreType.REGULAR((4,)),
            dma((9,)),
            dma,
            dma,
            dma,
            dma((chunks + 1,)),
            dma((3,)),
            dma((3,)),
            dma,
            dma((chunks,)),
            dma,
            dma((chunks,)),
            dma,
            dma,
            dma,
            dma,
            dma,
            dma,
            dma,
            dma,
        ],
        compiler_params=pltpu.CompilerParams(
            has_side_effects=True, collective_id=0, vmem_limit_bytes=VMEM_LIMIT
        ),
        name="sweep",
    )(
        keep(vol_curve),
        keep(bucket),
        keep(bump_size),
        keep(payoff.reshape(rows, LANES)),
        keep(positions.reshape(rows, LANES)),
        keep(offsets),
        keep(tiles),
        keep(lines),
    )
    groups = curves // SUB
    parts = max(1, rows // (4 * SUB))
    bumped, vega = pl.pallas_call(
        spread_kernel,
        out_shape=(
            jax.ShapeDtypeStruct((groups * rows * SUB, LANES), jnp.float32),
            jax.ShapeDtypeStruct((1, curves), jnp.float32),
        ),
        in_specs=[smem, smem, smem, vmem, vmem],
        out_specs=(pl.BlockSpec(memory_space=pl.ANY), pl.BlockSpec(memory_space=pl.ANY)),
        scratch_shapes=[
            pltpu.VMEM((groups * rows * SUB, LANES), jnp.float32),
            pltpu.VMEM((1, curves), jnp.float32),
            dma((parts, groups)),
            dma,
        ],
        compiler_params=pltpu.CompilerParams(vmem_limit_bytes=VMEM_LIMIT),
        name="spread",
    )(vol_on, bucket_on, bump_on, moved, sums)
    bumped = bumped.reshape(groups, rows, SUB, LANES).transpose(0, 2, 1, 3).reshape(curves, nodes)
    return bumped, vega.reshape(curves)


def solution(mesh):
    shape = dict(mesh.shape)
    in_specs = (
        P(("nx", "ny")),
        P(("nx", "ny")),
        P("bump", None, ("nx", "ny")),
        P(None, ("nx", "ny")),
        P(),
        P("bump"),
        P("bump"),
    )
    out_specs = (P("bump", ("nx", "ny")), P("bump"))
    body = functools.partial(on_device, shape["bump"], shape["nx"], shape["ny"])
    return jax.shard_map(body, mesh=mesh, in_specs=in_specs, out_specs=out_specs, check_vma=False)
```

```python
import functools

import jax
import jax.numpy as jnp
from jax import lax
from jax.experimental import pallas as pl
from jax.experimental.pallas import tpu as pltpu
from jax.sharding import PartitionSpec as P

LANES = 128
SUB = 8
VMEM_LIMIT = 24 * 1024 * 1024
MESH = pl.DeviceIdType.MESH


def sweep_kernel(
    dims,
    curve_ref,
    bucket_ref,
    bump_ref,
    payoff_ref,
    positions_ref,
    offsets_ref,
    tables_ref,
    rows_ref,
    sums_ref,
    vol_ref,
    picks_ref,
    sizes_ref,
    tab,
    pay,
    pos,
    offs,
    coef,
    state,
    mid,
    part,
    gathered,
    strip_sum,
    total,
    edge_out,
    edge_in,
    lent,
    hello,
    loc_sem,
    lent_send,
    lent_recv,
    tab_send,
    tab_recv,
    halo_send,
    halo_recv,
    mid_send,
    mid_recv,
    far_send,
    far_recv,
    near_send,
    near_recv,
    ring_send,
    ring_recv,
    strip_send,
    strip_recv,
    tot_send,
    tot_recv,
):
    n, nx, ny, steps, per, block_len, bounds, strip = dims
    ring_size = nx * ny
    rows = payoff_ref.shape[0]
    blocks = offsets_ref.shape[1]
    comps = tables_ref.shape[0]
    group = n // 2
    half = steps // 2
    share = rows // group
    chunks = len(bounds) - 1
    me = lax.axis_index("bump")
    ring = lax.axis_index("nx") * ny + lax.axis_index("ny")
    side = me // group
    core = lax.rem(me, group)
    upper = side == 1
    lower = side == 0
    first = core == 0

    def at(r, q):
        return {"bump": q, "nx": r // ny, "ny": lax.rem(r, ny)}

    right = lax.rem(ring + 1, ring_size)
    left = lax.rem(ring + ring_size - 1, ring_size)
    sibling = at(ring, side * group + (1 - core))
    across = at(ring, (1 - side) * group + core)
    diagonal = at(ring, (1 - side) * group + (1 - core))
    outer = at(jnp.where(first, right, left), me)

    def start_of(c, a, b):
        return pl.multiple_of(SUB + jnp.where(c == 0, share - b, a), SUB)

    def local(a, b):
        return pl.ds(start_of(core, a, b), b - a)

    def wide_at(c, a, b):
        return pl.ds(pl.multiple_of(start_of(c, a, b) + c * share, SUB), b - a)

    def owned_at(c, a, b):
        return pl.ds(pl.multiple_of(start_of(c, a, b) + c * share - SUB, SUB), b - a)

    def table_at(c, a, b):
        begin = (start_of(c, a, b) + c * share) * per
        return pl.ds(pl.multiple_of(begin, SUB * per), (b - a) * per)

    reach = bounds[1] + 2 * SUB

    def table_load(i, a, b):
        there = tab.at[core, :, (SUB + a) * per : (SUB + b) * per]
        return pltpu.make_async_copy(tables_ref.at[:, a * per : b * per], there, loc_sem.at[i])

    loads = [
        table_load(0, share - reach, share + reach),
        pltpu.make_async_copy(payoff_ref, pay.at[SUB : SUB + rows], loc_sem.at[1]),
        pltpu.make_async_copy(positions_ref, pos, loc_sem.at[2]),
        pltpu.make_async_copy(offsets_ref, offs.at[0], loc_sem.at[3]),
        pltpu.make_async_copy(curve_ref, vol_ref, loc_sem.at[4]),
        pltpu.make_async_copy(bucket_ref, picks_ref, loc_sem.at[5]),
        pltpu.make_async_copy(bump_ref, sizes_ref, loc_sem.at[6]),
        table_load(7, 0, share - reach),
        table_load(8, share + reach, rows),
    ]

    barrier = pltpu.get_barrier_semaphore()

    def greet(sem, to):
        pl.semaphore_signal(sem, inc=1, device_id=to, device_id_type=MESH)

    rest = jnp.logical_not(first)

    for copy in loads[:1] + loads[3:5]:
        copy.start()

    @pl.when(first)
    def _():
        greet(barrier, sibling)
        greet(barrier, at(left, group))

    @pl.when(rest)
    def _():
        greet(barrier, at(right, group))

    @pl.when(upper)
    def _():
        greet(barrier, at(ring, 1))
        loads[1].start()
        loads[2].start()

    for copy in loads[7:]:
        copy.start()

    @pl.when(lower)
    def _():
        for i in range(1, ring_size):
            greet(barrier, at(lax.rem(ring + i, ring_size), 0))
        loads[2].start()

    for copy in loads[5:7]:
        copy.start()

    @pl.when(jnp.logical_and(upper, rest))
    def _():
        pl.semaphore_wait(barrier, 1)
        greet(hello.at[0], sibling)

    @pl.when(jnp.logical_and(lower, rest))
    def _():
        pl.semaphore_wait(barrier, 3)
        greet(hello.at[0], sibling)
        greet(hello.at[1], across)
        greet(hello.at[1], diagonal)

    @pl.when(first)
    def _():
        pl.semaphore_wait(hello.at[0], 1)

    loads[0].wait()

    def remote(src, dst, send, recv, to):
        return pltpu.make_async_remote_copy(
            src_ref=src, dst_ref=dst, send_sem=send, recv_sem=recv, device_id=to, device_id_type=MESH
        )

    def fresh(j):
        lo = -SUB if j == 0 else min(bounds[j] + 2 * SUB, share)
        return lo, min(bounds[j + 1] + 2 * SUB, share)

    from_row, to_row = bounds[strip], bounds[strip + 1]
    lent_rows = to_row - from_row + 2

    lent_at = slice((SUB - 1) * per, (SUB - 1 + lent_rows) * per)

    def lend(c):
        begin = SUB + c * share + (share - to_row if c == 0 else from_row) - 1
        source = tab.at[core, :, begin * per : (begin + lent_rows) * per]
        to = at(ring, (1 - side) * group + c)
        return remote(source, lent.at[core, :, lent_at], lent_send, lent_recv, to)

    def all_of(ref, sem):
        pltpu.make_async_copy(ref, ref, sem).wait()

    pieces = [fresh(j) for j in range(chunks)]
    parts = [pieces[0], (pieces[1][0], pieces[2][1]), (pieces[3][0], share)]
    needed = {0: 0, 1: 1, 3: 2}
    table_copies = []
    for j, (lo, hi) in enumerate(parts):
        there = tab.at[core, :, table_at(1 - core, lo, hi)]
        table_copies.append(remote(there, there, tab_send, tab_recv.at[j], sibling))
    edge = pl.multiple_of(jnp.where(first, SUB, rows) * per, SUB * per)
    there = tab.at[core, :, pl.ds(edge, SUB * per)]
    table_copies.append(remote(there, there, tab_send, tab_recv.at[3], sibling))
    table_copies[0].start()
    loads[7].wait()
    loads[8].wait()

    @pl.when(lower)
    def _():
        for c in range(group):
            lend(c).start()

    for copy in table_copies[1:]:
        copy.start()

    def arrived(j):
        here = tab.at[1 - core, :, table_at(core, *parts[j])]
        return remote(here, here, tab_send, tab_recv.at[j], sibling)

    out_from = pl.multiple_of(jnp.where(first, rows, SUB), SUB)
    out_to = pl.multiple_of(jnp.where(first, 0, rows + SUB), SUB)
    halo_copies = [
        remote(
            pay.at[pl.ds(out_from, SUB)], pay.at[pl.ds(out_to, SUB)],
            halo_send.at[0], halo_recv.at[0], outer,
        ),
        remote(offs.at[0], offs.at[1], halo_send.at[1], halo_recv.at[1], outer),
        remote(edge_out, edge_in, halo_send.at[2], halo_recv.at[2], outer),
    ]

    lines = [(slot, k, (slot * comps + k) * per) for slot in range(group) for k in range(comps)]

    def gather_edge():
        taken = tab.at[1 - core, :, pl.ds(pl.multiple_of(out_from * per, SUB * per), SUB * per)]
        remote(taken, taken, tab_send, tab_recv.at[3], sibling).wait_recv()

        @pl.when(first)
        def _():
            for slot, k, line in lines:
                at_row = (SUB + rows - 1) * per
                edge_out[line : line + per, :] = tab[slot, k, at_row : at_row + per, :]

        @pl.when(rest)
        def _():
            for slot, k, line in lines:
                edge_out[line : line + per, :] = tab[slot, k, SUB * per : (SUB + 1) * per, :]

    def place_edge():
        @pl.when(first)
        def _():
            for slot, k, line in lines:
                at_row = (SUB - 1) * per
                tab[slot, k, at_row : at_row + per, :] = edge_in[line : line + per, :]

        @pl.when(rest)
        def _():
            for slot, k, line in lines:
                at_row = (SUB + rows) * per
                tab[slot, k, at_row : at_row + per, :] = edge_in[line : line + per, :]

    loads[3].wait()
    loads[4].wait()

    def prepare(a, b, source, borrowed=False):
        count = b - a
        begin = start_of(core, a, b)
        row = lax.broadcasted_iota(jnp.int32, (count, blocks), 0) + (begin - SUB + core * share + rows)
        hit = lax.broadcasted_iota(jnp.int32, (count, blocks), 1) == lax.rem(row, rows) * LANES // block_len
        here = pl.ds(begin, count)
        for t in range(half):
            step = t if borrowed else side * half + t
            slot, at_step = t // per, t % per
            line = offs[source, pl.ds(step, 1), :].astype(jnp.float32)
            branch = jnp.sum(jnp.where(hit, line, 0.0), axis=1, keepdims=True)
            branch = jnp.broadcast_to(branch, (count, LANES))
            low = branch < -0.5
            high = branch > 0.5

            def entry(k):
                if borrowed:
                    return lent[slot, k, pl.ds(at_step, count, stride=per), :]
                first_row = (begin + core * share) * per + at_step
                return tab[slot, k, pl.ds(first_row, count, stride=per), :]

            w = vol_ref[step] * vol_ref[step]
            discount = entry(0)
            slope_up = discount * entry(2)
            slope_down = discount * entry(4)
            up = discount * entry(1) + w * slope_up
            down = discount * entry(3) + w * slope_down
            middle = discount - up - down
            slope_mid = -slope_up - slope_down

            def put(k, above, level, below):
                zero = jnp.zeros_like(above)
                coef[t, k, here, :] = jnp.where(high, above, zero)
                coef[t, k + 1, here, :] = jnp.where(high, level, jnp.where(low, zero, above))
                coef[t, k + 2, here, :] = jnp.where(high, below, jnp.where(low, above, level))
                coef[t, k + 3, here, :] = jnp.where(high, zero, jnp.where(low, level, below))
                coef[t, k + 4, here, :] = jnp.where(low, below, zero)

            put(0, up, middle, down)
            put(5, slope_up, slope_mid, slope_down)

    def advance(a, b, top):
        count = b - a
        here = local(a, b)
        lane = lax.broadcasted_iota(jnp.int32, (count, LANES), 1)
        for t in reversed(range(half)):
            s = top + t
            c = [coef[t, k, here, :] for k in range(5)]
            for g in [0] + list(range(s + 2, steps + 1)):
                x = state[g, 0:count, :]
                after = pltpu.roll(x, count - 1, 0)
                before = pltpu.roll(x, 1, 0)
                f1 = pltpu.roll(jnp.where(lane < 1, after, x), LANES - 1, 1)
                f2 = pltpu.roll(jnp.where(lane < 2, after, x), LANES - 2, 1)
                b1 = pltpu.roll(jnp.where(lane >= LANES - 1, before, x), 1, 1)
                b2 = pltpu.roll(jnp.where(lane >= LANES - 2, before, x), 2, 1)
                state[g, 0:count, :] = c[0] * f2 + c[1] * f1 + c[2] * x + c[3] * b1 + c[4] * b2
                if g == 0:
                    e = [coef[t, 5 + k, here, :] for k in range(5)]
                    state[s + 1, 0:count, :] = e[0] * f2 + e[1] * f1 + e[2] * x + e[3] * b1 + e[4] * b2

    passed = [0] + list(range(half + 1, steps + 1))

    def mid_piece(j):
        return (-SUB if j == 0 else bounds[j] + SUB), bounds[j + 1] + SUB

    def mid_rows(j):
        lo = -1 if j == 0 else bounds[j] + 1
        hi = bounds[j + 1] + 1
        return (hi - 2 if j == strip else lo), hi

    mid_total = sum(hi - lo for lo, hi in map(mid_rows, range(chunks)))

    def mid_copy(j, c):
        lo, hi = mid_rows(j)
        begin = SUB + (share - hi if c == 0 else lo)
        here = mid.at[:, begin : begin + hi - lo]
        return remote(here, here, mid_send, mid_recv.at[j], across)

    def each_core(act):
        @pl.when(first)
        def _():
            act(0)

        @pl.when(rest)
        def _():
            act(1)

    def result_at(c, j):
        return rows_ref.at[:, owned_at(c, bounds[j], bounds[j + 1])]

    def far_copy(j):
        here = result_at(core, j)
        return remote(here, here, far_send, far_recv.at[j], across)

    def near_copy(j):
        here = result_at(core, j)
        return remote(here, here, near_send, near_recv, sibling)

    def weigh(g, here, fresh):
        weighted = jnp.sum(pos[here, :] * rows_ref[g, here, :], axis=0, keepdims=True)
        part[g - 1 : g, :] = weighted if fresh else part[g - 1 : g, :] + weighted

    def packed():
        each = jnp.broadcast_to(jnp.sum(part[...], axis=1, keepdims=True), (steps, LANES))
        place = lax.broadcasted_iota(jnp.int32, (steps, LANES), 0)
        lane = lax.broadcasted_iota(jnp.int32, (steps, LANES), 1)
        return jnp.sum(jnp.where(place == lane, each, 0.0), axis=0, keepdims=True)

    strip_copy = remote(strip_sum.at[0], strip_sum.at[1], strip_send, strip_recv, across)
    def total_copy(to):
        return remote(total.at[0], total.at[1], tot_send, tot_recv, to)


    mine = rows_ref.at[:, owned_at(core, 0, share)]
    others = rows_ref.at[:, owned_at(1 - core, 0, share)]

    wrapped = lax.axis_index("ny") == 0

    def send_halos():
        gather_edge()

        @pl.when(first)
        def _():
            pl.semaphore_wait(barrier, 4)
            greet(hello.at[2], sibling)
            greet(hello.at[2], across)
            greet(hello.at[2], diagonal)

        @pl.when(rest)
        def _():
            pl.semaphore_wait(hello.at[2], 1)

        for copy in halo_copies:
            copy.start()

    def send_lower_halos():
        pl.semaphore_wait(hello.at[2], 1)
        for copy in halo_copies[1:]:
            copy.start()

    @pl.when(upper)
    def _():
        loads[1].wait()
        for j in range(chunks):
            lo, hi = mid_piece(j)
            begin, end = max(lo - SUB, -SUB), min(hi + SUB, share + SUB)
            if j in needed:
                arrived(needed[j]).wait_recv()
            if pieces[j][0] < pieces[j][1]:
                prepare(*pieces[j], 0)
            if j == chunks - 1:
                pl.when(wrapped)(send_halos)
                for copy in halo_copies:
                    copy.wait_recv()
                place_edge()
                prepare(share, share + SUB, 1)
            count = end - begin
            state[0, 0:count, :] = pay[wide_at(core, begin, end), :]
            advance(begin, end, half)
            shift = pl.multiple_of(jnp.where(first, end - hi, lo - begin), SUB)
            for i, g in enumerate(passed):
                mid[i, local(lo, hi), :] = state[g, pl.ds(shift, hi - lo), :]
            if j == 0:
                pl.semaphore_wait(hello.at[1], 1)
            each_core(lambda c: mid_copy(j, c).start())
            if j == 1:
                pl.when(jnp.logical_not(wrapped))(send_halos)
        loads[2].wait()
        all_of(lent.at[:, :, lent_at], lent_recv)
        begin, end = from_row - SUB, to_row + SUB
        prepare(begin, end, 0, True)
        for i, g in enumerate(passed):
            state[g, 0 : end - begin, :] = mid[i, local(begin, end), :]
        advance(begin, end, 0)
        for g in range(steps + 1):
            rows_ref[g, owned_at(core, from_row, to_row), :] = state[g, SUB : end - begin - SUB, :]
            if g:
                weigh(g, owned_at(core, from_row, to_row), True)
        strip_sum[0] = packed()
        strip_copy.start()
        far_copy(strip).start()
        near_copy(strip).start()
        for copy in halo_copies:
            copy.wait_send()
        for j in range(chunks):
            if j != strip:
                far_copy(j).wait_recv()
                near_copy(j).start()
        total_copy(across).wait_recv()
        sums_ref[...] = total[1]
        strip_copy.wait_send()
        all_of(mid.at[:, 0:mid_total], mid_send)
        far_copy(strip).wait_send()

    @pl.when(lower)
    def _():
        loads[2].wait()
        gather_edge()
        for j in range(chunks):
            if j in needed:
                arrived(needed[j]).wait_recv()
            if pieces[j][0] < pieces[j][1]:
                prepare(*pieces[j], 0)
        for j in range(chunks):
            lo, hi = bounds[j], bounds[j + 1]
            begin, end = lo - SUB, hi + SUB
            if j == 0:
                pl.when(jnp.logical_not(wrapped))(send_lower_halos)
            if j == 2:
                pl.when(wrapped)(send_lower_halos)
            if j == strip:
                mid_copy(j, 0).wait_recv()

                @pl.when(first)
                def _():
                    pl.semaphore_wait(barrier, 2 * ring_size - 2)
                    greet(hello.at[3], sibling)

                continue
            if j == chunks - 1:
                for copy in halo_copies[1:]:
                    copy.wait_recv()
                place_edge()
                prepare(share, share + SUB, 1)
            mid_copy(j, 0).wait_recv()
            count = end - begin

            def take(c):
                skip = SUB - 1
                start = share - hi if c == 0 else lo
                a, b = (skip, count) if c == 0 else (0, count - skip)
                for i, g in enumerate(passed):
                    state[g, a:b, :] = mid[i, start + a : start + b, :]

            each_core(take)
            advance(begin, end, 0)
            here = owned_at(core, lo, hi)
            for g in range(steps + 1):
                rows_ref[g, here, :] = state[g, SUB : SUB + hi - lo, :]
            far_copy(j).start()
            near_copy(j).start()
            for g in range(1, steps + 1):
                weigh(g, here, j == 0)

        strip_copy.wait_recv()
        own = core * ring_size + ring
        gathered[own] = packed() + strip_sum[1]

        @pl.when(rest)
        def _():
            pl.semaphore_wait(hello.at[3], 1)

        for i in range(1, ring_size):
            for c in range(group):
                to = at(lax.rem(ring + i, ring_size), c)
                remote(gathered.at[own], gathered.at[own], ring_send, ring_recv, to).start()
        remote(gathered.at[own], gathered.at[own], ring_send, ring_recv, sibling).start()
        far_copy(strip).wait_recv()
        near_copy(strip).start()
        all_of(gathered.at[1 : group * ring_size], ring_recv)
        total[0] = jnp.sum(gathered[...], axis=0)

        @pl.when(rest)
        def _():
            total_copy(across).start()
            total_copy(diagonal).start()

        sums_ref[...] = total[0]
        all_of(gathered.at[1 : group * ring_size], ring_send)

        @pl.when(rest)
        def _():
            all_of(gathered.at[0:2], tot_send)

        for copy in halo_copies[1:]:
            copy.wait_send()
        all_of(rows_ref.at[:, owned_at(core, 0, share - (to_row - from_row))], far_send)
        all_of(lent.at[:, :, lent_at], lent_send)

    all_of(others, near_recv)
    all_of(mine, near_send)
    all_of(tab.at[core, :, 0 : (share + 2 * SUB) * per], tab_send)
    loads[5].wait()
    loads[6].wait()

def spread_kernel(
    vol_ref, bucket_ref, bump_ref, rows_ref, sums_ref, out_ref, vega_ref, held, small, sem, small_sem
):
    curves = bucket_ref.shape[0]
    groups = curves // SUB
    rows = rows_ref.shape[1]
    parts = max(1, rows // (4 * SUB))
    span = rows // parts
    picks = []
    for b in range(curves):
        s = bucket_ref[b]
        slope = 2.0 * vol_ref[s] + bump_ref[b]
        picks.append((s, slope, bump_ref[b] * slope))
    for i in range(parts):
        here = slice(i * span, (i + 1) * span)
        base = rows_ref[0, here, :]
        for b in range(curves):
            s, _, change = picks[b]
            line = (b // SUB * rows + i * span) * SUB + b % SUB
            held[pl.ds(line, span, stride=SUB), :] = base + change * rows_ref[s + 1, here, :]
        for g in range(groups):
            place = slice((g * rows + i * span) * SUB, (g * rows + (i + 1) * span) * SUB)
            pltpu.make_async_copy(held.at[place], out_ref.at[place], sem).start()
        if i == 0:
            lane = lax.broadcasted_iota(jnp.int32, (1, curves), 1)
            spot = lax.broadcasted_iota(jnp.int32, (1, LANES), 1)
            total = jnp.zeros((1, curves), jnp.float32)
            for b in range(curves):
                s, slope, _ = picks[b]
                weighted = jnp.sum(jnp.where(spot == s, sums_ref[...], 0.0), axis=1, keepdims=True)
                total = jnp.where(lane == b, slope * weighted, total)
            small[...] = total
            vega_copy = pltpu.make_async_copy(small, vega_ref, small_sem)
            vega_copy.start()
    vega_copy.wait()
    pltpu.make_async_copy(held, out_ref, sem).wait()


def on_device(n, nx, ny, payoff, positions, tables, offsets, vol_curve, bucket, bump_size):
    steps = vol_curve.shape[0]
    per, comps, nodes = tables.shape
    curves = bucket.shape[0]
    rows = nodes // LANES
    block_len = nodes // offsets.shape[1]
    group = n // 2
    share = rows // group
    half = steps // 2
    ring = nx * ny
    bounds = [share * k // (16 * SUB) * SUB for k in (0, 1, 3, 6, 10, 12, 14, 16)]
    strip = 4
    chunks = len(bounds) - 1
    widest = max(b - a for a, b in zip(bounds, bounds[1:])) + 3 * SUB
    tiles = tables.transpose(1, 0, 2).reshape(comps, per, rows, LANES).transpose(0, 2, 1, 3)
    tiles = tiles.reshape(comps, rows * per, LANES)
    dma = pltpu.SemaphoreType.DMA
    vmem = pl.BlockSpec(memory_space=pltpu.VMEM)
    smem = pl.BlockSpec(memory_space=pltpu.SMEM)
    hbm = pl.BlockSpec(memory_space=pltpu.HBM)

    def keep(x):
        return pltpu.with_memory_space_constraint(x, pltpu.HBM)

    moved, sums, vol_on, bucket_on, bump_on = pl.pallas_call(
        functools.partial(sweep_kernel, (n, nx, ny, steps, per, block_len, bounds, strip)),
        out_shape=(
            pltpu.VMEM((steps + 1, rows, LANES), jnp.float32),
            pltpu.VMEM((1, LANES), jnp.float32),
            pltpu.SMEM(vol_curve.shape, vol_curve.dtype),
            pltpu.SMEM(bucket.shape, bucket.dtype),
            pltpu.SMEM(bump_size.shape, bump_size.dtype),
        ),
        in_specs=[hbm] * 7,
        out_specs=(vmem, vmem, smem, smem, smem),
        scratch_shapes=[
            pltpu.VMEM((group, comps, (rows + 2 * SUB) * per, LANES), jnp.float32),
            pltpu.VMEM((rows + 2 * SUB, LANES), jnp.float32),
            pltpu.VMEM((rows, LANES), jnp.float32),
            pltpu.VMEM((2,) + offsets.shape, jnp.int32),
            pltpu.VMEM((half, 10, share + 2 * SUB, LANES), jnp.float32),
            pltpu.VMEM((steps + 1, widest, LANES), jnp.float32),
            pltpu.VMEM((half + 1, share + 2 * SUB, LANES), jnp.float32),
            pltpu.VMEM((steps, LANES), jnp.float32),
            pltpu.VMEM((group * ring, 1, LANES), jnp.float32),
            pltpu.VMEM((2, 1, LANES), jnp.float32),
            pltpu.VMEM((2, 1, LANES), jnp.float32),
            pltpu.VMEM((group * comps * per, LANES), jnp.float32),
            pltpu.VMEM((group * comps * per, LANES), jnp.float32),
            pltpu.VMEM(
                (group, comps, (bounds[strip + 1] - bounds[strip] + 2 * SUB) * per, LANES), jnp.float32
            ),
            pltpu.SemaphoreType.REGULAR((4,)),
            dma((9,)),
            dma,
            dma,
            dma,
            dma((4,)),
            dma((3,)),
            dma((3,)),
            dma,
            dma((chunks,)),
            dma,
            dma((chunks,)),
            dma,
            dma,
            dma,
            dma,
            dma,
            dma,
            dma,
            dma,
        ],
        compiler_params=pltpu.CompilerParams(
            has_side_effects=True, collective_id=0, vmem_limit_bytes=VMEM_LIMIT
        ),
        name="sweep",
    )(
        keep(vol_curve),
        keep(bucket),
        keep(bump_size),
        keep(payoff.reshape(rows, LANES)),
        keep(positions.reshape(rows, LANES)),
        keep(offsets),
        keep(tiles),
    )
    groups = curves // SUB
    bumped, vega = pl.pallas_call(
        spread_kernel,
        out_shape=(
            jax.ShapeDtypeStruct((groups * rows * SUB, LANES), jnp.float32),
            jax.ShapeDtypeStruct((1, curves), jnp.float32),
        ),
        in_specs=[smem, smem, smem, vmem, vmem],
        out_specs=(pl.BlockSpec(memory_space=pl.ANY), pl.BlockSpec(memory_space=pl.ANY)),
        scratch_shapes=[
            pltpu.VMEM((groups * rows * SUB, LANES), jnp.float32),
            pltpu.VMEM((1, curves), jnp.float32),
            dma,
            dma,
        ],
        compiler_params=pltpu.CompilerParams(vmem_limit_bytes=VMEM_LIMIT),
        name="spread",
    )(vol_on, bucket_on, bump_on, moved, sums)
    bumped = bumped.reshape(groups, rows, SUB, LANES).transpose(0, 2, 1, 3).reshape(curves, nodes)
    return bumped, vega.reshape(curves)


def solution(mesh):
    shape = dict(mesh.shape)
    in_specs = (
        P(("nx", "ny")),
        P(("nx", "ny")),
        P("bump", None, ("nx", "ny")),
        P(None, ("nx", "ny")),
        P(),
        P("bump"),
        P("bump"),
    )
    out_specs = (P("bump", ("nx", "ny")), P("bump"))
    body = functools.partial(on_device, shape["bump"], shape["nx"], shape["ny"])
    return jax.shard_map(body, mesh=mesh, in_specs=in_specs, out_specs=out_specs, check_vma=False)
```

```python
import functools

import jax
import jax.numpy as jnp
from jax import lax
from jax.experimental import pallas as pl
from jax.experimental.pallas import tpu as pltpu
from jax.sharding import PartitionSpec as P

LANES = 128
SUB = 8
VMEM_LIMIT = 24 * 1024 * 1024
MESH = pl.DeviceIdType.MESH


def sweep_kernel(
    dims,
    curve_ref,
    bucket_ref,
    bump_ref,
    payoff_ref,
    positions_ref,
    offsets_ref,
    tables_ref,
    rows_ref,
    sums_ref,
    vol_ref,
    picks_ref,
    sizes_ref,
    tab,
    pay,
    pos,
    offs,
    coef,
    state,
    mid,
    part,
    gathered,
    strip_sum,
    total,
    edge_out,
    edge_in,
    lent,
    hello,
    loc_sem,
    lent_sem,
    tab_send,
    tab_recv,
    halo_send,
    halo_recv,
    mid_send,
    far_send,
    cross_recv,
    near_send,
    near_recv,
    ring_send,
    ring_recv,
    sum_send,
    sum_recv,
):
    n, nx, ny, steps, per, block_len, bounds, strip = dims
    ring_size = nx * ny
    rows = payoff_ref.shape[0]
    blocks = offsets_ref.shape[1]
    comps = tables_ref.shape[0]
    group = n // 2
    half = steps // 2
    share = rows // group
    chunks = len(bounds) - 1
    me = lax.axis_index("bump")
    ring = lax.axis_index("nx") * ny + lax.axis_index("ny")
    side = me // group
    core = lax.rem(me, group)
    upper = side == 1
    lower = side == 0
    first = core == 0

    def at(r, q):
        return {"bump": q, "nx": r // ny, "ny": lax.rem(r, ny)}

    right = lax.rem(ring + 1, ring_size)
    left = lax.rem(ring + ring_size - 1, ring_size)
    sibling = at(ring, side * group + (1 - core))
    across = at(ring, (1 - side) * group + core)
    diagonal = at(ring, (1 - side) * group + (1 - core))
    outer = at(jnp.where(first, right, left), me)

    def start_of(c, a, b):
        return pl.multiple_of(SUB + jnp.where(c == 0, share - b, a), SUB)

    def local(a, b):
        return pl.ds(start_of(core, a, b), b - a)

    def wide_at(c, a, b):
        return pl.ds(pl.multiple_of(start_of(c, a, b) + c * share, SUB), b - a)

    def owned_at(c, a, b):
        return pl.ds(pl.multiple_of(start_of(c, a, b) + c * share - SUB, SUB), b - a)

    def table_at(c, a, b):
        begin = (start_of(c, a, b) + c * share) * per
        return pl.ds(pl.multiple_of(begin, SUB * per), (b - a) * per)

    reach = bounds[1] + 2 * SUB

    def table_load(i, a, b):
        there = tab.at[core, :, (SUB + a) * per : (SUB + b) * per]
        return pltpu.make_async_copy(tables_ref.at[:, a * per : b * per], there, loc_sem.at[i])

    loads = [
        table_load(0, share - reach, share + reach),
        pltpu.make_async_copy(payoff_ref, pay.at[SUB : SUB + rows], loc_sem.at[1]),
        pltpu.make_async_copy(positions_ref, pos, loc_sem.at[2]),
        pltpu.make_async_copy(offsets_ref, offs.at[0], loc_sem.at[3]),
        pltpu.make_async_copy(curve_ref, vol_ref, loc_sem.at[4]),
        pltpu.make_async_copy(bucket_ref, picks_ref, loc_sem.at[5]),
        pltpu.make_async_copy(bump_ref, sizes_ref, loc_sem.at[6]),
        table_load(7, 0, share - reach),
        table_load(7, share + reach, rows),
    ]

    barrier = pltpu.get_barrier_semaphore()

    def greet(sem, to):
        pl.semaphore_signal(sem, inc=1, device_id=to, device_id_type=MESH)

    rest = jnp.logical_not(first)

    for copy in loads[:1] + loads[3:5]:
        copy.start()

    @pl.when(first)
    def _():
        greet(barrier, sibling)
        greet(barrier, at(left, group))

    @pl.when(rest)
    def _():
        greet(barrier, at(right, group))

    @pl.when(upper)
    def _():
        greet(barrier, at(ring, 1))
        loads[1].start()
        loads[2].start()

    for copy in loads[7:]:
        copy.start()

    @pl.when(lower)
    def _():
        for i in range(1, ring_size):
            greet(barrier, at(lax.rem(ring + i, ring_size), 0))
        loads[2].start()

    for copy in loads[5:7]:
        copy.start()

    @pl.when(jnp.logical_and(upper, rest))
    def _():
        pl.semaphore_wait(barrier, 1)
        greet(hello.at[0], sibling)

    @pl.when(jnp.logical_and(lower, rest))
    def _():
        pl.semaphore_wait(barrier, 3)
        greet(hello.at[0], sibling)
        greet(hello.at[1], across)
        greet(hello.at[1], diagonal)

    @pl.when(first)
    def _():
        pl.semaphore_wait(hello.at[0], 1)

    loads[0].wait()

    def remote(src, dst, send, recv, to):
        return pltpu.make_async_remote_copy(
            src_ref=src, dst_ref=dst, send_sem=send, recv_sem=recv, device_id=to, device_id_type=MESH
        )

    def fresh(j):
        lo = -SUB if j == 0 else min(bounds[j] + 2 * SUB, share)
        return lo, min(bounds[j + 1] + 2 * SUB, share)

    from_row, to_row = bounds[strip], bounds[strip + 1]
    lent_rows = to_row - from_row + 2

    lent_at = slice((SUB - 1) * per, (SUB - 1 + lent_rows) * per)

    def lend(c):
        begin = SUB + c * share + (share - to_row if c == 0 else from_row) - 1
        source = tab.at[core, :, begin * per : (begin + lent_rows) * per]
        to = at(ring, (1 - side) * group + c)
        return remote(source, lent.at[core, :, lent_at], lent_sem, lent_sem, to)

    def all_of(ref, sem):
        pltpu.make_async_copy(ref, ref, sem).wait()

    pieces = [fresh(j) for j in range(chunks)]
    parts = [pieces[0], (pieces[1][0], pieces[2][1]), (pieces[3][0], share)]
    needed = {0: 0, 1: 1, 3: 2}
    table_copies = []
    for j, (lo, hi) in enumerate(parts):
        there = tab.at[core, :, table_at(1 - core, lo, hi)]
        table_copies.append(remote(there, there, tab_send, tab_recv.at[j], sibling))
    edge = pl.multiple_of(jnp.where(first, SUB, rows) * per, SUB * per)
    there = tab.at[core, :, pl.ds(edge, SUB * per)]
    table_copies.append(remote(there, there, tab_send, tab_recv.at[3], sibling))
    table_copies[0].start()
    all_of(tab.at[core, :, 0 : (rows - 2 * reach) * per], loc_sem.at[7])

    @pl.when(lower)
    def _():
        for c in range(group):
            lend(c).start()

    for copy in table_copies[1:]:
        copy.start()

    def arrived(j):
        here = tab.at[1 - core, :, table_at(core, *parts[j])]
        return remote(here, here, tab_send, tab_recv.at[j], sibling)

    out_from = pl.multiple_of(jnp.where(first, rows, SUB), SUB)
    out_to = pl.multiple_of(jnp.where(first, 0, rows + SUB), SUB)
    halo_copies = [
        remote(
            pay.at[pl.ds(out_from, SUB)], pay.at[pl.ds(out_to, SUB)],
            halo_send, halo_recv.at[0], outer,
        ),
        remote(offs.at[0], offs.at[1], halo_send, halo_recv.at[1], outer),
        remote(edge_out, edge_in, halo_send, halo_recv.at[2], outer),
    ]

    lines = [(slot, k, (slot * comps + k) * per) for slot in range(group) for k in range(comps)]

    def gather_edge():
        taken = tab.at[1 - core, :, pl.ds(pl.multiple_of(out_from * per, SUB * per), SUB * per)]
        remote(taken, taken, tab_send, tab_recv.at[3], sibling).wait_recv()

        @pl.when(first)
        def _():
            for slot, k, line in lines:
                at_row = (SUB + rows - 1) * per
                edge_out[line : line + per, :] = tab[slot, k, at_row : at_row + per, :]

        @pl.when(rest)
        def _():
            for slot, k, line in lines:
                edge_out[line : line + per, :] = tab[slot, k, SUB * per : (SUB + 1) * per, :]

    def place_edge():
        @pl.when(first)
        def _():
            for slot, k, line in lines:
                at_row = (SUB - 1) * per
                tab[slot, k, at_row : at_row + per, :] = edge_in[line : line + per, :]

        @pl.when(rest)
        def _():
            for slot, k, line in lines:
                at_row = (SUB + rows) * per
                tab[slot, k, at_row : at_row + per, :] = edge_in[line : line + per, :]

    loads[3].wait()
    loads[4].wait()

    def prepare(a, b, source, borrowed=False):
        count = b - a
        begin = start_of(core, a, b)
        row = lax.broadcasted_iota(jnp.int32, (count, blocks), 0) + (begin - SUB + core * share + rows)
        hit = lax.broadcasted_iota(jnp.int32, (count, blocks), 1) == lax.rem(row, rows) * LANES // block_len
        here = pl.ds(begin, count)
        for t in range(half):
            step = t if borrowed else side * half + t
            slot, at_step = t // per, t % per
            line = offs[source, pl.ds(step, 1), :].astype(jnp.float32)
            branch = jnp.sum(jnp.where(hit, line, 0.0), axis=1, keepdims=True)
            branch = jnp.broadcast_to(branch, (count, LANES))
            low = branch < -0.5
            high = branch > 0.5

            def entry(k):
                if borrowed:
                    return lent[slot, k, pl.ds(at_step, count, stride=per), :]
                first_row = (begin + core * share) * per + at_step
                return tab[slot, k, pl.ds(first_row, count, stride=per), :]

            w = vol_ref[step] * vol_ref[step]
            discount = entry(0)
            slope_up = discount * entry(2)
            slope_down = discount * entry(4)
            up = discount * entry(1) + w * slope_up
            down = discount * entry(3) + w * slope_down
            middle = discount - up - down
            slope_mid = -slope_up - slope_down

            def put(k, above, level, below):
                zero = jnp.zeros_like(above)
                coef[t, k, here, :] = jnp.where(high, above, zero)
                coef[t, k + 1, here, :] = jnp.where(high, level, jnp.where(low, zero, above))
                coef[t, k + 2, here, :] = jnp.where(high, below, jnp.where(low, above, level))
                coef[t, k + 3, here, :] = jnp.where(high, zero, jnp.where(low, level, below))
                coef[t, k + 4, here, :] = jnp.where(low, below, zero)

            put(0, up, middle, down)
            put(5, slope_up, slope_mid, slope_down)

    def advance(a, b, top):
        count = b - a
        here = local(a, b)
        lane = lax.broadcasted_iota(jnp.int32, (count, LANES), 1)
        for t in reversed(range(half)):
            s = top + t
            c = [coef[t, k, here, :] for k in range(5)]
            for g in [0] + list(range(s + 2, steps + 1)):
                x = state[g, 0:count, :]
                after = pltpu.roll(x, count - 1, 0)
                before = pltpu.roll(x, 1, 0)
                f1 = pltpu.roll(jnp.where(lane < 1, after, x), LANES - 1, 1)
                f2 = pltpu.roll(jnp.where(lane < 2, after, x), LANES - 2, 1)
                b1 = pltpu.roll(jnp.where(lane >= LANES - 1, before, x), 1, 1)
                b2 = pltpu.roll(jnp.where(lane >= LANES - 2, before, x), 2, 1)
                state[g, 0:count, :] = c[0] * f2 + c[1] * f1 + c[2] * x + c[3] * b1 + c[4] * b2
                if g == 0:
                    e = [coef[t, 5 + k, here, :] for k in range(5)]
                    state[s + 1, 0:count, :] = e[0] * f2 + e[1] * f1 + e[2] * x + e[3] * b1 + e[4] * b2

    passed = [0] + list(range(half + 1, steps + 1))

    def mid_piece(j):
        return (-SUB if j == 0 else bounds[j] + SUB), bounds[j + 1] + SUB

    def mid_rows(j):
        lo = -1 if j == 0 else bounds[j] - 1 if j == strip + 1 else bounds[j] + 1
        return lo, bounds[j + 1] + 1

    sent = [j for j in range(chunks) if j != strip]
    mid_total = sum(hi - lo for lo, hi in map(mid_rows, sent))

    def mid_copy(j, c):
        lo, hi = mid_rows(j)
        begin = SUB + (share - hi if c == 0 else lo)
        here = mid.at[:, begin : begin + hi - lo]
        return remote(here, here, mid_send, cross_recv.at[j], across)

    def each_core(act):
        @pl.when(first)
        def _():
            act(0)

        @pl.when(rest)
        def _():
            act(1)

    def result_at(c, j):
        return rows_ref.at[:, owned_at(c, bounds[j], bounds[j + 1])]

    def far_copy(j):
        here = result_at(core, j)
        return remote(here, here, far_send, cross_recv.at[j], across)

    def near_copy(j):
        here = result_at(core, j)
        return remote(here, here, near_send, near_recv, sibling)

    def weigh(g, here, fresh):
        weighted = jnp.sum(pos[here, :] * rows_ref[g, here, :], axis=0, keepdims=True)
        part[g - 1 : g, :] = weighted if fresh else part[g - 1 : g, :] + weighted

    def packed():
        each = jnp.broadcast_to(jnp.sum(part[...], axis=1, keepdims=True), (steps, LANES))
        place = lax.broadcasted_iota(jnp.int32, (steps, LANES), 0)
        lane = lax.broadcasted_iota(jnp.int32, (steps, LANES), 1)
        return jnp.sum(jnp.where(place == lane, each, 0.0), axis=0, keepdims=True)

    strip_copy = remote(strip_sum.at[0], strip_sum.at[1], sum_send, sum_recv, across)
    def total_copy(to):
        return remote(total.at[0], total.at[1], sum_send, sum_recv, to)


    mine = rows_ref.at[:, owned_at(core, 0, share)]
    others = rows_ref.at[:, owned_at(1 - core, 0, share)]

    wrapped = lax.axis_index("ny") == 0
    halo_rows = steps * blocks // LANES + group * comps * per

    def send_halos():
        gather_edge()

        @pl.when(first)
        def _():
            pl.semaphore_wait(barrier, 4)
            greet(hello.at[2], sibling)
            greet(hello.at[2], across)
            greet(hello.at[2], diagonal)

        @pl.when(rest)
        def _():
            pl.semaphore_wait(hello.at[2], 1)

        for copy in halo_copies:
            copy.start()

    def send_lower_halos():
        pl.semaphore_wait(hello.at[2], 1)
        for copy in halo_copies[1:]:
            copy.start()

    @pl.when(upper)
    def _():
        loads[1].wait()
        for j in range(chunks):
            lo, hi = mid_piece(j)
            begin, end = max(lo - SUB, -SUB), min(hi + SUB, share + SUB)
            if j in needed:
                arrived(needed[j]).wait_recv()
            if pieces[j][0] < pieces[j][1]:
                prepare(*pieces[j], 0)
            if j == chunks - 1:
                pl.when(wrapped)(send_halos)
                for copy in halo_copies:
                    copy.wait_recv()
                place_edge()
                prepare(share, share + SUB, 1)
            count = end - begin
            state[0, 0:count, :] = pay[wide_at(core, begin, end), :]
            advance(begin, end, half)
            shift = pl.multiple_of(jnp.where(first, end - hi, lo - begin), SUB)
            for i, g in enumerate(passed):
                mid[i, local(lo, hi), :] = state[g, pl.ds(shift, hi - lo), :]
            if j == 0:
                pl.semaphore_wait(hello.at[1], 1)
            if j != strip:
                each_core(lambda c: mid_copy(j, c).start())
            if j == 1:
                pl.when(jnp.logical_not(wrapped))(send_halos)
        loads[2].wait()
        all_of(lent.at[:, :, lent_at], lent_sem)
        begin, end = from_row - SUB, to_row + SUB
        prepare(begin, end, 0, True)
        for i, g in enumerate(passed):
            state[g, 0 : end - begin, :] = mid[i, local(begin, end), :]
        advance(begin, end, 0)
        for g in range(steps + 1):
            rows_ref[g, owned_at(core, from_row, to_row), :] = state[g, SUB : end - begin - SUB, :]
            if g:
                weigh(g, owned_at(core, from_row, to_row), True)
        strip_sum[0] = packed()
        strip_copy.start()
        far_copy(strip).start()
        near_copy(strip).start()
        all_of(pay.at[0 : SUB + halo_rows], halo_send)
        for j in range(chunks):
            if j != strip:
                far_copy(j).wait_recv()
                near_copy(j).start()
        total_copy(across).wait_recv()
        sums_ref[...] = total[1]
        strip_copy.wait_send()
        all_of(mid.at[:, 0:mid_total], mid_send)
        far_copy(strip).wait_send()

    @pl.when(lower)
    def _():
        loads[2].wait()
        gather_edge()
        for j in range(chunks):
            if j in needed:
                arrived(needed[j]).wait_recv()
            if pieces[j][0] < pieces[j][1]:
                prepare(*pieces[j], 0)
        for j in range(chunks):
            lo, hi = bounds[j], bounds[j + 1]
            begin, end = lo - SUB, hi + SUB
            if j == 0:
                pl.when(jnp.logical_not(wrapped))(send_lower_halos)
            if j == 2:
                pl.when(wrapped)(send_lower_halos)
            if j == strip:

                @pl.when(first)
                def _():
                    pl.semaphore_wait(barrier, 2 * ring_size - 2)
                    greet(hello.at[1], sibling)

                continue
            if j == chunks - 1:
                for copy in halo_copies[1:]:
                    copy.wait_recv()
                place_edge()
                prepare(share, share + SUB, 1)
            mid_copy(j, 0).wait_recv()
            count = end - begin

            def take(c):
                skip = SUB - 1
                start = share - hi if c == 0 else lo
                a, b = (skip, count) if c == 0 else (0, count - skip)
                for i, g in enumerate(passed):
                    state[g, a:b, :] = mid[i, start + a : start + b, :]

            each_core(take)
            advance(begin, end, 0)
            here = owned_at(core, lo, hi)
            for g in range(steps + 1):
                rows_ref[g, here, :] = state[g, SUB : SUB + hi - lo, :]
            far_copy(j).start()
            near_copy(j).start()
            for g in range(1, steps + 1):
                weigh(g, here, j == 0)

        strip_copy.wait_recv()
        own = core * ring_size + ring
        gathered[own] = packed() + strip_sum[1]

        @pl.when(rest)
        def _():
            pl.semaphore_wait(hello.at[1], 1)

        for i in range(1, ring_size):
            for c in range(group):
                to = at(lax.rem(ring + i, ring_size), c)
                remote(gathered.at[own], gathered.at[own], ring_send, ring_recv, to).start()
        remote(gathered.at[own], gathered.at[own], ring_send, ring_recv, sibling).start()
        far_copy(strip).wait_recv()
        near_copy(strip).start()
        all_of(gathered.at[1 : group * ring_size], ring_recv)
        total[0] = jnp.sum(gathered[...], axis=0)

        @pl.when(rest)
        def _():
            total_copy(across).start()
            total_copy(diagonal).start()

        sums_ref[...] = total[0]
        all_of(gathered.at[1 : group * ring_size], ring_send)

        @pl.when(rest)
        def _():
            all_of(gathered.at[0:2], sum_send)

        all_of(pay.at[0:halo_rows], halo_send)
        all_of(rows_ref.at[:, owned_at(core, 0, share - (to_row - from_row))], far_send)
        all_of(lent.at[:, :, lent_at], lent_sem)

    all_of(others, near_recv)
    all_of(mine, near_send)
    all_of(tab.at[core, :, 0 : (share + 2 * SUB) * per], tab_send)
    loads[5].wait()
    loads[6].wait()

def spread_kernel(
    vol_ref, bucket_ref, bump_ref, rows_ref, sums_ref, out_ref, vega_ref, held, small, sem, small_sem
):
    curves = bucket_ref.shape[0]
    groups = curves // SUB
    rows = rows_ref.shape[1]
    parts = max(1, rows // (4 * SUB))
    span = rows // parts
    picks = []
    for b in range(curves):
        s = bucket_ref[b]
        slope = 2.0 * vol_ref[s] + bump_ref[b]
        picks.append((s, slope, bump_ref[b] * slope))
    for i in range(parts):
        here = slice(i * span, (i + 1) * span)
        base = rows_ref[0, here, :]
        for b in range(curves):
            s, _, change = picks[b]
            line = (b // SUB * rows + i * span) * SUB + b % SUB
            held[pl.ds(line, span, stride=SUB), :] = base + change * rows_ref[s + 1, here, :]
        for g in range(groups):
            place = slice((g * rows + i * span) * SUB, (g * rows + (i + 1) * span) * SUB)
            pltpu.make_async_copy(held.at[place], out_ref.at[place], sem).start()
        if i == 0:
            lane = lax.broadcasted_iota(jnp.int32, (1, curves), 1)
            spot = lax.broadcasted_iota(jnp.int32, (1, LANES), 1)
            total = jnp.zeros((1, curves), jnp.float32)
            for b in range(curves):
                s, slope, _ = picks[b]
                weighted = jnp.sum(jnp.where(spot == s, sums_ref[...], 0.0), axis=1, keepdims=True)
                total = jnp.where(lane == b, slope * weighted, total)
            small[...] = total
            vega_copy = pltpu.make_async_copy(small, vega_ref, small_sem)
            vega_copy.start()
    vega_copy.wait()
    pltpu.make_async_copy(held, out_ref, sem).wait()


def on_device(n, nx, ny, payoff, positions, tables, offsets, vol_curve, bucket, bump_size):
    steps = vol_curve.shape[0]
    per, comps, nodes = tables.shape
    curves = bucket.shape[0]
    rows = nodes // LANES
    block_len = nodes // offsets.shape[1]
    group = n // 2
    share = rows // group
    half = steps // 2
    ring = nx * ny
    bounds = [share * k // (16 * SUB) * SUB for k in (0, 1, 2, 4, 7, 10, 12, 14, 16)]
    strip = 5
    chunks = len(bounds) - 1
    widest = max(b - a for a, b in zip(bounds, bounds[1:])) + 3 * SUB
    tiles = tables.transpose(1, 0, 2).reshape(comps, per, rows, LANES).transpose(0, 2, 1, 3)
    tiles = tiles.reshape(comps, rows * per, LANES)
    dma = pltpu.SemaphoreType.DMA
    vmem = pl.BlockSpec(memory_space=pltpu.VMEM)
    smem = pl.BlockSpec(memory_space=pltpu.SMEM)
    hbm = pl.BlockSpec(memory_space=pltpu.HBM)

    def keep(x):
        return pltpu.with_memory_space_constraint(x, pltpu.HBM)

    moved, sums, vol_on, bucket_on, bump_on = pl.pallas_call(
        functools.partial(sweep_kernel, (n, nx, ny, steps, per, block_len, bounds, strip)),
        out_shape=(
            pltpu.VMEM((steps + 1, rows, LANES), jnp.float32),
            pltpu.VMEM((1, LANES), jnp.float32),
            pltpu.SMEM(vol_curve.shape, vol_curve.dtype),
            pltpu.SMEM(bucket.shape, bucket.dtype),
            pltpu.SMEM(bump_size.shape, bump_size.dtype),
        ),
        in_specs=[hbm] * 7,
        out_specs=(vmem, vmem, smem, smem, smem),
        scratch_shapes=[
            pltpu.VMEM((group, comps, (rows + 2 * SUB) * per, LANES), jnp.float32),
            pltpu.VMEM((rows + 2 * SUB, LANES), jnp.float32),
            pltpu.VMEM((rows, LANES), jnp.float32),
            pltpu.VMEM((2,) + offsets.shape, jnp.int32),
            pltpu.VMEM((half, 10, share + 2 * SUB, LANES), jnp.float32),
            pltpu.VMEM((steps + 1, widest, LANES), jnp.float32),
            pltpu.VMEM((half + 1, share + 2 * SUB, LANES), jnp.float32),
            pltpu.VMEM((steps, LANES), jnp.float32),
            pltpu.VMEM((group * ring, 1, LANES), jnp.float32),
            pltpu.VMEM((2, 1, LANES), jnp.float32),
            pltpu.VMEM((2, 1, LANES), jnp.float32),
            pltpu.VMEM((group * comps * per, LANES), jnp.float32),
            pltpu.VMEM((group * comps * per, LANES), jnp.float32),
            pltpu.VMEM(
                (group, comps, (bounds[strip + 1] - bounds[strip] + 2 * SUB) * per, LANES), jnp.float32
            ),
            pltpu.SemaphoreType.REGULAR((3,)),
            dma((8,)),
            dma,
            dma,
            dma((4,)),
            dma,
            dma((3,)),
            dma,
            dma,
            dma((chunks,)),
            dma,
            dma,
            dma,
            dma,
            dma,
            dma,
        ],
        compiler_params=pltpu.CompilerParams(
            has_side_effects=True, collective_id=0, vmem_limit_bytes=VMEM_LIMIT
        ),
        name="sweep",
    )(
        keep(vol_curve),
        keep(bucket),
        keep(bump_size),
        keep(payoff.reshape(rows, LANES)),
        keep(positions.reshape(rows, LANES)),
        keep(offsets),
        keep(tiles),
    )
    groups = curves // SUB
    bumped, vega = pl.pallas_call(
        spread_kernel,
        out_shape=(
            jax.ShapeDtypeStruct((groups * rows * SUB, LANES), jnp.float32),
            jax.ShapeDtypeStruct((1, curves), jnp.float32),
        ),
        in_specs=[smem, smem, smem, vmem, vmem],
        out_specs=(pl.BlockSpec(memory_space=pl.ANY), pl.BlockSpec(memory_space=pl.ANY)),
        scratch_shapes=[
            pltpu.VMEM((groups * rows * SUB, LANES), jnp.float32),
            pltpu.VMEM((1, curves), jnp.float32),
            dma,
            dma,
        ],
        compiler_params=pltpu.CompilerParams(vmem_limit_bytes=VMEM_LIMIT),
        name="spread",
    )(vol_on, bucket_on, bump_on, moved, sums)
    bumped = bumped.reshape(groups, rows, SUB, LANES).transpose(0, 2, 1, 3).reshape(curves, nodes)
    return bumped, vega.reshape(curves)


def solution(mesh):
    shape = dict(mesh.shape)
    in_specs = (
        P(("nx", "ny")),
        P(("nx", "ny")),
        P("bump", None, ("nx", "ny")),
        P(None, ("nx", "ny")),
        P(),
        P("bump"),
        P("bump"),
    )
    out_specs = (P("bump", ("nx", "ny")), P("bump"))
    body = functools.partial(on_device, shape["bump"], shape["nx"], shape["ny"])
    return jax.shard_map(body, mesh=mesh, in_specs=in_specs, out_specs=out_specs, check_vma=False)
```
